512 devices in a mesh: xz: 64 (over y, x, core), gy: 8 (over z).
Axes of the slice: x: 4, y: 8, z: 8, core: 2. Of those that a mesh axis runs over, the one named last changes fastest.
Arguments:
- initial_state: float32 [3, 2, 64, 512, 512], P(None, None, 'gy', 'xz'), may hold values from -6 to 6
- drag_rate: float32 [64, 512, 1024], P('gy', 'xz'), may hold values from 0.02 to 0.6
- wall_control: float32 [512, 1024], P('xz'), may hold values from -6 to 6
- lift_profile: float32 [64], replicated, may hold values from 0.05 to 0.3
- schur_inverse: float32 [64, 8, 512, 512], P('gy', None, 'xz'), may hold values from -1 to 3, as said below
Outputs:
- final_state: float32 [3, 2, 64, 512, 512], P(None, None, 'gy', 'xz')
- control_gradient: float32 [512, 1024], P('xz', 'gy')
The draws below stay inside these ranges and needn't reach their ends.
Inputs may be any that keep to these rules, and one draw needn't show every extreme that they name: `schur_inverse`: each 8 x 8 block of one wavenumber holds the precomputed inverse of a Schur complement; dimension 1 indexes the block's columns.
All inputs are finite; a program needn't handle non-finite values.
Results may differ from the reference program's by a relative error of at most 0.00014.
Values sent between devices are 32-bit elements; how exact they have to be, the bound alone decides.
A program may use at most 128 MiB of HBM per device.

```python
import math
import jax
import jax.numpy as jnp
from jax import lax

NX = 1024
NZ = 512
KX = 512
CY = 8
NY = 64
STEPS = 2
N_GY = 8


def draw_schur_inverse(key, part):
    subkeys = jax.random.split(key, 4)
    blocks = NY // CY
    full_shape = (blocks, CY, CY, NX // 2, NZ)
    diag_low = 0.4
    rank_weight = 0.6
    spread = 0.5
    diagonal = jax.random.uniform(subkeys[0], (blocks, CY, 1, NX // 2, NZ), jnp.float32, diag_low, 1.0)
    identity = (jnp.arange(CY)[:, None] == jnp.arange(CY)[None, :]).astype(jnp.float32)[None, :, :, None, None]
    jitter = jax.random.uniform(subkeys[1], full_shape, jnp.float32, -1.0, 1.0) * (spread / math.sqrt(CY))
    left_side = jax.random.uniform(subkeys[2], (blocks, CY, 1, NX // 2, NZ), jnp.float32, 0.5, 1.0)
    right_side = jax.random.uniform(subkeys[3], (blocks, 1, CY, NX // 2, NZ), jnp.float32, 0.5, 1.0)
    blocked = identity * diagonal + jitter + rank_weight * left_side * right_side
    stream_wave = 2.0 * math.pi / NX * jnp.arange(NX // 2).astype(jnp.float32)
    span_ids = jnp.arange(NZ)
    signed = jnp.where(span_ids < NZ // 2, span_ids, span_ids - NZ)
    span_wave = jnp.where(span_ids == NZ // 2, 0.0, 2.0 * math.pi / NZ * signed.astype(jnp.float32))
    damping = 1.0 + stream_wave[:, None] ** 2 + span_wave[None, :] ** 2
    return (blocked / damping).reshape(NY, CY, NX // 2, NZ)


def level_of(own_key, extent, cuts, least, top_value):
    gain = 1.0
    for axis_at, blocks in cuts:
        steps = jax.random.uniform(jax.random.fold_in(jax.random.fold_in(own_key, 6), axis_at), (blocks,), jnp.float32, least / len(cuts), top_value / len(cuts))
        gain = gain * jnp.repeat(jnp.exp(steps), extent[axis_at] // blocks).reshape((-1,) + (1,) * (len(extent) - 1 - axis_at))
    return gain


def gaussian(rng, shape, width, reach, cuts=(), dtype=jnp.bfloat16):
    level = level_of(rng, shape, cuts, -0.22, 0.18) if cuts else 1.0
    entries = jax.random.normal(rng, shape, jnp.float32) * width * level
    return jnp.minimum(jnp.maximum(entries, -reach), reach).astype(dtype)


def setup_inputs(seed: int = 0) -> dict:
    seeds = jax.random.split(jax.random.key(seed), 6)
    return {
        "initial_state": gaussian(seeds[0], (3, 2, NY, KX, NZ), 1.0, 6.0, ((2, 8), (3, 64)), jnp.float32),
        "drag_rate": jnp.clip(jnp.exp(math.log(0.6) - 3.4011974 * jax.random.uniform(seeds[1], (NY, NZ, NX), jnp.float32) ** level_of(seeds[1], (NY, NZ, NX), ((0, 8), (1, 64)), -0.2, 0.2)), 0.02, 0.6),
        "wall_control": gaussian(seeds[2], (NZ, NX), 1.0, 6.0, ((0, 64),), jnp.float32),
        "lift_profile": jnp.clip(jnp.exp(jax.random.uniform(seeds[3], (NY,), jnp.float32, math.log(0.05), math.log(0.3))), 0.05, 0.3),
        "schur_inverse": draw_schur_inverse(jax.random.fold_in(seeds[5], 71), 0),
    }


DIFFUSION = 0.04

def pair_rotate(spectrum, factor):
    return jnp.stack([-factor * spectrum[1], factor * spectrum[0]])

def reference(initial_state, drag_rate, wall_control, lift_profile, schur_inverse):
    mode_ids = jnp.arange(KX)
    stream_factor = (2.0 * math.pi / NX * mode_ids.astype(jnp.float32))[:, None]
    span_ids = jnp.arange(NZ)
    signed = jnp.where(span_ids < NZ // 2, span_ids, span_ids - NZ)
    span_wave = jnp.where(span_ids == NZ // 2, 0.0, 2.0 * math.pi / NZ * signed.astype(jnp.float32))
    wave_square = stream_factor ** 2 + span_wave[None, :] ** 2

    def to_physical(spectral):
        values = lax.complex(spectral[0], spectral[1])
        values = jnp.fft.ifft(values, axis=2, norm='ortho')
        values = jnp.swapaxes(values, 1, 2)
        values = jnp.pad(values, ((0, 0), (0, 0), (0, 1)))
        return jnp.fft.irfft(values, n=NX, axis=2, norm='ortho')

    def to_spectral(physical):
        values = jnp.fft.rfft(physical, axis=2, norm='ortho')[:, :, :KX]
        values = jnp.swapaxes(values, 1, 2)
        values = jnp.fft.fft(values, axis=2, norm='ortho')
        return jnp.stack([jnp.real(values), jnp.imag(values)])

    def curvature(spectrum):
        padded = jnp.pad(spectrum, ((0, 0), (1, 1), (0, 0), (0, 0)))
        return padded[:, 2:] - 2.0 * spectrum + padded[:, :-2]

    def centred(spectrum):
        padded = jnp.pad(spectrum, ((0, 0), (1, 1), (0, 0), (0, 0)))
        return (padded[:, 2:] - padded[:, :-2]) / 2.0

    def solve(source):
        running = jnp.zeros((2, KX, NZ), jnp.float32)
        partials = []
        for block_index in range(N_GY):
            matrix = schur_inverse[block_index * CY:(block_index + 1) * CY]
            values = source[:, block_index * CY:(block_index + 1) * CY]
            summed = jnp.einsum('ijkq,cjkq->cikq', matrix, values, precision=lax.Precision.HIGHEST)
            partial_value = summed + matrix[:, 0][None] * running[:, None]
            running = partial_value[:, CY - 1]
            partials.append(partial_value)
        running = jnp.zeros((2, KX, NZ), jnp.float32)
        solved = [None] * N_GY
        for block_index in reversed(range(N_GY)):
            matrix = schur_inverse[block_index * CY:(block_index + 1) * CY]
            complete = partials[block_index] + matrix[:, CY - 1][None] * running[:, None]
            running = complete[:, 0]
            solved[block_index] = complete
        return jnp.concatenate(solved, axis=1)

    def evolve(control_plane):
        control_hat = to_spectral(control_plane[None])[:, 0]
        fields = initial_state
        for section_index in range(STEPS):
            stream_part = fields[0]
            normal_part = fields[1]
            span_part = fields[2]
            drag_term = to_spectral(drag_rate * to_physical(stream_part))
            stream_star = stream_part + DIFFUSION * (curvature(stream_part) - wave_square * stream_part) - drag_term
            normal_star = normal_part + DIFFUSION * (curvature(normal_part) - wave_square * normal_part) + lift_profile[:, None, None] * control_hat[:, None]
            span_star = span_part + DIFFUSION * (curvature(span_part) - wave_square * span_part)
            divergence = pair_rotate(stream_star, stream_factor) + centred(normal_star) + pair_rotate(span_star, span_wave)
            pressure = solve(divergence)
            fields = jnp.stack([stream_star - pair_rotate(pressure, stream_factor), normal_star - centred(pressure), span_star - pair_rotate(pressure, span_wave)])
        return fields
    final_state, pullback = jax.vjp(evolve, wall_control)
    control_gradient = pullback(final_state)[0]
    return (final_state, control_gradient)
```

```python
import functools
import math

import jax
import jax.numpy as jnp
import numpy as np
from jax import lax
from jax.experimental import pallas as pl
from jax.experimental.pallas import tpu as pltpu
from jax.sharding import PartitionSpec as P

MESH = pl.DeviceIdType.MESH
F32 = jnp.float32
BF16 = jnp.bfloat16
DIFFUSION = 0.04
NX = 1024
NZ = 512
KX = 512
ROWS = 8
MODES = 8
PEERS = 64
SLABS = 8
ROUNDS = 4
CONTROL_SLOT = 6
FINAL_SLOT = 7


def base_table(period, scale):
    k = np.arange(512)
    high = 2.0 * np.pi * ((32 * np.arange(16)[:, None] * k) % period) / period
    low = 2.0 * np.pi * ((np.arange(32)[:, None] * k) % period) / period
    return np.concatenate(
        [np.cos(high), np.sin(high), np.cos(low) * scale, np.sin(low) * scale]
    ).astype(np.float32)


def split(x):
    hi = x.astype(BF16)
    return hi, (x - hi.astype(F32))


def butterfly(tiles, lane):
    tiles = list(tiles)
    for bit in range(4):
        step = 1 << bit
        shift = 8 * step
        upper = (lane // shift) % 2 == 1
        for a in range(16):
            if a & step == 0:
                x, y = tiles[a], tiles[a | step]
                tiles[a] = jnp.where(upper, pltpu.roll(y, shift, 1), x)
                tiles[a | step] = jnp.where(upper, y, pltpu.roll(x, 128 - shift, 1))
    return tiles


def kernel(
    state_in, drag_in, ctrl_in, lift_ref, schur, base_x, base_z,
    out_state, out_grad,
    st, pu, pv, pw, divb, direct, pbuf, wall, chat, zin, zout,
    tx, tzh, tzl, dg, waves, amat,
    send, recv, hsend, hrecv, ssend, srecv, gsend, grecv, fsend, frecv,
    send_sem, recv_sem, hsend_sem, hrecv_sem, ssend_sem, srecv_sem, misc_sem,
):
    me = lax.axis_index("xz")
    slab = lax.axis_index("gy")
    barrier = pltpu.get_barrier_semaphore()

    @pl.loop(1, PEERS)
    def _(i):
        pl.semaphore_signal(
            barrier, inc=1, device_id=(lax.rem(me + i, PEERS), slab), device_id_type=MESH
        )

    @pl.loop(1, SLABS)
    def _(i):
        pl.semaphore_signal(
            barrier, inc=1, device_id=(me, lax.rem(slab + i, SLABS)), device_id_type=MESH
        )

    lane = lax.broadcasted_iota(jnp.int32, (8, 128), 1)
    wide_lane = lax.broadcasted_iota(jnp.int32, (KX, 128), 1)
    left = wide_lane < 64
    odd = lax.broadcasted_iota(jnp.int32, (KX, 128), 0) % 2 == 1

    mode = me * MODES + lax.broadcasted_iota(jnp.int32, (MODES, NZ), 0)
    span = lax.broadcasted_iota(jnp.int32, (MODES, NZ), 1)
    kx = (2.0 * math.pi / NX) * mode.astype(F32)
    signed = jnp.where(span < NZ // 2, span, span - NZ)
    kz = jnp.where(span == NZ // 2, 0.0, (2.0 * math.pi / NZ) * signed.astype(F32))
    waves[0] = kx
    waves[1] = kz
    waves[2] = kx * kx + kz * kz
    waves[3] = jnp.where(mode == 0, 1.0, 2.0).astype(F32)

    @pl.loop(0, 16)
    def _(i):
        rows = pl.ds(pl.multiple_of(i * 32, 32), 32)
        for base, which in ((base_x, 0), (base_z, 1)):
            ca = base[pl.ds(i, 1), :]
            sa = base[pl.ds(16 + i, 1), :]
            cb = base[32:64, :]
            sb = base[64:96, :]
            c_hi, c_lo = split(ca * cb - sa * sb)
            s_hi, s_lo = split(sa * cb + ca * sb)
            if which == 0:
                tx[rows, 0:512] = c_hi
                tx[rows, 512:1024] = c_lo.astype(BF16)
                tx[rows, 1024:1536] = s_hi
                tx[rows, 1536:2048] = s_lo.astype(BF16)
            else:
                tzh[rows, 0:512] = c_hi
                tzh[rows, 512:1024] = s_hi
                tzl[rows, 0:512] = c_lo.astype(BF16)
                tzl[rows, 512:1024] = s_lo.astype(BF16)

    for b in range(4):
        lo = drag_in[:, :, 128 * b : 128 * b + 128].reshape(64, 128)
        hi = drag_in[:, :, 512 + 128 * b : 640 + 128 * b].reshape(64, 128)
        dg[128 * b : 128 * b + 128, :] = jnp.concatenate([lo, hi], axis=0).T

    for comp in range(3):
        for c in range(2):
            @pl.loop(0, ROWS)
            def _(y):
                st[comp, y + 2, c] = state_in[comp, c, y]

    gsend[0] = schur[0, 0]
    gsend[1] = schur[0, 7]
    gsend[2] = schur[7, 0]
    gsend[3] = schur[7, 7]

    def x_inverse(slot):
        value = recv[slot].reshape(KX, 128)
        hi = value.astype(BF16).astype(F32)
        lo = value - hi
        real = jnp.where(left, hi, pltpu.roll(lo, 64, 1))
        imag = -jnp.where(left, pltpu.roll(hi, 64, 1), lo)
        rc = jnp.concatenate([real, jnp.where(odd, -real, real)], axis=1).astype(BF16)
        rs = jnp.concatenate([imag, jnp.where(odd, -imag, imag)], axis=1).astype(BF16)
        out = jnp.dot(tx[:, 0:512], rc, preferred_element_type=F32)
        out += jnp.dot(tx[:, 512:1024], rc, preferred_element_type=F32)
        out += jnp.dot(tx[:, 1024:1536], rs, preferred_element_type=F32)
        out += jnp.dot(tx[:, 1536:2048], rs, preferred_element_type=F32)
        near, far = out[:, 0:128], out[:, 128:256]
        near = near + pltpu.roll(near, 64, 1)
        far = far + pltpu.roll(far, 64, 1)
        return jnp.where(left, near, far)

    def x_forward(value, slot):
        turned = pltpu.roll(value, 64, 1)
        total = value + turned
        gap = jnp.where(left, value - turned, turned - value)

        def packed(part):
            hi = part.astype(BF16).astype(F32)
            return jnp.where(left, hi, part - hi)

        ra = jnp.concatenate([packed(total), packed(gap)], axis=1).astype(BF16)
        with_cos = jnp.dot(tx[:, 0:512], ra, preferred_element_type=F32)
        with_cos += jnp.dot(tx[:, 512:1024], ra, preferred_element_type=F32)
        with_sin = jnp.dot(tx[:, 1024:1536], ra, preferred_element_type=F32)
        with_sin += jnp.dot(tx[:, 1536:2048], ra, preferred_element_type=F32)

        def folded(part):
            part = jnp.where(odd, part[:, 128:256], part[:, 0:128])
            return part + pltpu.roll(part, 64, 1)

        result = jnp.where(left, folded(with_cos), -folded(with_sin))
        send[slot] = result.reshape(PEERS, 8, 128)

    def z_dot(value):
        hi, lo = split(value)
        both = jnp.concatenate([hi, lo.astype(BF16)], axis=0)
        out = jnp.dot(both, tzh[...], preferred_element_type=F32)
        out = out[0:128] + out[128:256]
        out += jnp.dot(hi, tzl[...], preferred_element_type=F32)
        out = out.reshape(ROWS, 2, MODES, 1024)
        return out[:, :, :, 0:512], out[:, :, :, 512:1024]

    def z_inverse(value, slot):
        with_cos, with_sin = z_dot(value)
        zout[:, 0] = with_cos[:, 0] - with_sin[:, 1]
        zout[:, 1] = with_sin[:, 0] + with_cos[:, 1]

        @pl.loop(0, 4)
        def _(j):
            lanes = pl.ds(pl.multiple_of(j * 128, 128), 128)
            tiles = [zout[a % 8, a // 8, :, lanes] for a in range(16)]
            for g, tile in enumerate(butterfly(tiles, lane)):
                send[slot, j * 16 + g] = tile

    def z_forward(slot):
        @pl.loop(0, 4)
        def _(j):
            lanes = pl.ds(pl.multiple_of(j * 128, 128), 128)
            tiles = [recv[slot, j * 16 + g] for g in range(16)]
            for a, tile in enumerate(butterfly(tiles, lane)):
                zin[a % 8, a // 8, :, lanes] = tile

        with_cos, with_sin = z_dot(zin[...].reshape(128, NZ))
        zout[:, 0] = with_cos[:, 0] + with_sin[:, 1]
        zout[:, 1] = with_cos[:, 1] - with_sin[:, 0]

    def exchange(slot):
        @pl.loop(1, PEERS)
        def _(i):
            peer = lax.rem(me + i, PEERS)
            pltpu.make_async_remote_copy(
                src_ref=send.at[slot, peer],
                dst_ref=recv.at[slot, me],
                send_sem=send_sem.at[slot],
                recv_sem=recv_sem.at[slot],
                device_id=(peer, slab),
                device_id_type=MESH,
            ).start()

        recv[slot, me] = send[slot, me]

    def arrived(slot):
        whole = recv.at[slot, pl.ds(0, PEERS - 1)]
        pltpu.make_async_copy(whole, whole, recv_sem.at[slot]).wait()

    def left_device(buffer, sem, count):
        whole = buffer.at[pl.ds(0, count)]
        pltpu.make_async_copy(whole, whole, sem).wait()

    def to_slabs(source, target, out_sem, in_sem):
        @pl.loop(1, SLABS)
        def _(i):
            peer = lax.rem(slab + i, SLABS)
            pltpu.make_async_remote_copy(
                src_ref=source(peer),
                dst_ref=target,
                send_sem=out_sem,
                recv_sem=in_sem,
                device_id=(me, peer),
                device_id_type=MESH,
            ).start()

    for b in range(4):
        near = ctrl_in[:, 128 * b : 128 * b + 128]
        far = ctrl_in[:, 512 + 128 * b : 640 + 128 * b]
        blank = jnp.zeros((56, 128), F32)
        pieces = jnp.concatenate([near, blank, far, blank], axis=0)
        zin_rows = pieces.T
        wall_rows = pl.ds(128 * b, 128)
        send[FINAL_SLOT, 16 * b : 16 * b + 16] = zin_rows.reshape(16, 8, 128)
        del wall_rows
    x_forward(send[FINAL_SLOT].reshape(KX, 128), CONTROL_SLOT)

    pl.semaphore_wait(barrier, PEERS - 1 + SLABS - 1)

    to_slabs(lambda peer: gsend, grecv.at[slab], misc_sem.at[0], misc_sem.at[1])
    wall[...] = jnp.zeros_like(wall)

    @pl.loop(0, ROUNDS)
    def _(r):
        adjoint = r // 2
        moving = r != 2
        rate = jnp.where(moving, DIFFUSION, 0.0).astype(F32)

        @pl.when(moving)
        def _():
            before = jnp.where(r < 2, waves[3], 1.0)
            z_inverse((st[0, 2:10] * before).reshape(128, NZ), 2 * jnp.where(r == 3, 2, r))

        for side, (u_row, v_row) in enumerate(((9, 8), (2, 2))):
            hsend[r, side, 0] = st[0, u_row]
            hsend[r, side, 1] = st[1, v_row]
            hsend[r, side, 2] = st[1, v_row + 1]
            hsend[r, side, 3] = st[2, u_row]
        for side in range(2):
            peer = lax.rem(slab + (1 if side == 0 else SLABS - 1), SLABS)
            pltpu.make_async_remote_copy(
                src_ref=hsend.at[r, side],
                dst_ref=hrecv.at[r, side],
                send_sem=hsend_sem.at[r, side],
                recv_sem=hrecv_sem.at[r, side],
                device_id=(me, peer),
                device_id_type=MESH,
            ).start()

        @pl.when(moving)
        def _():
            exchange(2 * jnp.where(r == 3, 2, r))

        @pl.when(r == 0)
        def _():
            exchange(CONTROL_SLOT)

        for side in range(2):
            whole = hrecv.at[r, side]
            pltpu.make_async_copy(whole, whole, hrecv_sem.at[r, side]).wait()
        for side, (u_row, v_row, edge) in enumerate(((1, 0, 0), (10, 10, SLABS - 1))):
            open_side = slab != edge
            st[0, u_row] = jnp.where(open_side, hrecv[r, side, 0], 0.0)
            st[1, v_row] = jnp.where(open_side, hrecv[r, side, 1], 0.0)
            st[1, v_row + 1] = jnp.where(open_side, hrecv[r, side, 2], 0.0)
            st[2, u_row] = jnp.where(open_side, hrecv[r, side, 3], 0.0)

        square = waves[2]

        def diffused(comp, row):
            middle = st[comp, row]
            around = st[comp, row + 1] - 2.0 * middle + st[comp, row - 1]
            return middle + rate * (around - square * middle)

        @pl.loop(0, ROWS)
        def _(y):
            pu[y] = diffused(0, y + 2)
            pw[y] = diffused(2, y + 2)

        @pl.loop(0, ROWS + 2)
        def _(y):
            row = slab * ROWS + y - 1
            inside = jnp.logical_and(row >= 0, row < ROWS * SLABS)
            pv[y] = jnp.where(inside, diffused(1, y + 1), 0.0)

        @pl.when(moving)
        def _():
            slot = 2 * jnp.where(r == 3, 2, r)
            arrived(slot)
            x_forward(x_inverse(slot) * dg[...], slot + 1)
            exchange(slot + 1)

        @pl.when(r == 0)
        def _():
            arrived(CONTROL_SLOT)
            z_forward(CONTROL_SLOT)
            chat[...] = zout[0]
            pltpu.make_async_copy(
                grecv.at[pl.ds(0, SLABS - 1)], grecv.at[pl.ds(0, SLABS - 1)], misc_sem.at[1]
            ).wait()

            def gather_a(i, a):
                b = SLABS - 1 - i
                return grecv[b, 0] + grecv[b, 1] * a * grecv[b, 2]

            amat[...] = lax.fori_loop(0, SLABS - 1 - slab, gather_a, jnp.zeros((MODES, NZ), F32))

        @pl.when(r < 2)
        def _():
            @pl.loop(0, ROWS + 2)
            def _(y):
                row = slab * ROWS + y - 1
                inside = jnp.logical_and(row >= 0, row < ROWS * SLABS)
                safe = jnp.clip(row, 0, ROWS * SLABS - 1)
                level = jnp.where(inside, lift_ref[safe], 0.0)
                pv[y] = pv[y] + level * chat[...]

        kxv, kzv = waves[0], waves[1]

        @pl.when(moving)
        def _():
            slot = 2 * jnp.where(r == 3, 2, r) + 1
            arrived(slot)
            z_forward(slot)
            after = jnp.where(r < 2, 1.0, waves[3])

            @pl.loop(0, ROWS)
            def _(y):
                pu[y] = pu[y] - zout[y] * after

        @pl.loop(0, ROWS)
        def _(y):
            slope = 0.5 * (pv[y + 2] - pv[y])
            divb[y, 0] = slope[0] - kxv * pu[y, 1] - kzv * pw[y, 1]
            divb[y, 1] = slope[1] + kxv * pu[y, 0] + kzv * pw[y, 0]

        def entry(i, j):
            return schur[i + adjoint * (j - i), j + adjoint * (i - j)]

        @pl.loop(0, ROWS)
        def _(i):
            total = entry(i, 0) * divb[0]
            for j in range(1, ROWS):
                total = total + entry(i, j) * divb[j]
            direct[i] = total

        ratio = entry(7, 0)
        turn = entry(0, 7)
        last = direct[7]
        ssend[r, 0] = last
        ssend[r, 1] = direct[0] + turn * (amat[...] * last)
        to_slabs(
            lambda peer: ssend.at[r, jnp.where(peer > slab, 0, 1)],
            srecv.at[r, slab],
            ssend_sem.at[r],
            srecv_sem.at[r],
        )
        whole = srecv.at[r, pl.ds(0, SLABS - 1)]
        pltpu.make_async_copy(whole, whole, srecv_sem.at[r]).wait()

        blank = jnp.zeros((2, MODES, NZ), F32)
        entering = lax.fori_loop(
            0, slab, lambda b, z: srecv[r, b] + grecv[b, 2 - adjoint] * z, blank
        )

        def suffix(i, e):
            b = SLABS - 1 - i
            return srecv[r, b] + grecv[b, 1 + adjoint] * e

        above = lax.fori_loop(0, SLABS - 1 - slab, suffix, blank)
        leaving = above + amat[...] * (last + ratio * entering)
        pbuf[9] = leaving

        @pl.loop(0, ROWS)
        def _(i):
            pbuf[i + 1] = direct[i] + entry(i, 0) * entering + entry(i, 7) * leaving

        below = grecv[lax.max(slab - 1, 0), 3]
        pbuf[0] = jnp.where(slab == 0, 0.0, entering + below * pbuf[1])

        @pl.loop(0, ROWS)
        def _(y):
            p0, p1 = pbuf[y + 1, 0], pbuf[y + 1, 1]
            st[0, y + 2, 0] = pu[y, 0] + kxv * p1
            st[0, y + 2, 1] = pu[y, 1] - kxv * p0
            st[2, y + 2, 0] = pw[y, 0] + kzv * p1
            st[2, y + 2, 1] = pw[y, 1] - kzv * p0
            normal = pv[y + 1] - 0.5 * (pbuf[y + 2] - pbuf[y])
            st[1, y + 2] = normal
            level = jnp.where(r >= 2, lift_ref[slab * ROWS + y], 0.0)
            wall[...] = wall[...] + level * normal

        @pl.when(r == 1)
        def _():
            @pl.loop(0, ROWS)
            def _(y):
                for comp in range(3):
                    for c in range(2):
                        out_state[comp, c, y] = st[comp, y + 2, c]

    zin[...] = jnp.zeros_like(zin)
    zin[0] = wall[...]
    z_inverse(zin[...].reshape(128, NZ), FINAL_SLOT)
    exchange(FINAL_SLOT)
    arrived(FINAL_SLOT)
    plane = x_inverse(FINAL_SLOT)
    for b in range(4):
        turned = plane[128 * b : 128 * b + 128, :].T
        fsend[b] = turned[0:8]
        fsend[4 + b] = turned[64:72]
    to_slabs(
        lambda peer: fsend.at[peer], frecv.at[slab], misc_sem.at[2], misc_sem.at[3]
    )
    frecv[slab] = fsend[slab]
    left_device(frecv, misc_sem.at[3], SLABS - 1)
    total = frecv[0]
    for b in range(1, SLABS):
        total = total + frecv[b]
    out_grad[...] = total

    @pl.loop(0, 8)
    def _(slot):
        left_device(send.at[slot], send_sem.at[slot], PEERS - 1)

    @pl.loop(0, ROUNDS)
    def _(r):
        for side in range(2):
            whole = hsend.at[r, side]
            pltpu.make_async_copy(whole, whole, hsend_sem.at[r, side]).wait()
        left_device(srecv.at[r], ssend_sem.at[r], SLABS - 1)

    left_device(grecv, misc_sem.at[0], SLABS - 1)
    left_device(frecv, misc_sem.at[2], SLABS - 1)


def per_device(initial_state, drag_rate, wall_control, lift_profile, schur_inverse):
    row = (2, MODES, NZ)
    vmem = pl.BlockSpec(memory_space=pltpu.VMEM)
    smem = pl.BlockSpec(memory_space=pltpu.SMEM)
    dma = pltpu.SemaphoreType.DMA
    return pl.pallas_call(
        kernel,
        out_shape=(
            jax.ShapeDtypeStruct((3, 2, ROWS, MODES, NZ), F32),
            jax.ShapeDtypeStruct((8, 128), F32),
        ),
        in_specs=[vmem, vmem, vmem, smem, vmem, vmem, vmem],
        out_specs=(vmem, vmem),
        scratch_shapes=[
            pltpu.VMEM((3, ROWS + 4, *row), F32),
            pltpu.VMEM((ROWS, *row), F32),
            pltpu.VMEM((ROWS + 2, *row), F32),
            pltpu.VMEM((ROWS, *row), F32),
            pltpu.VMEM((ROWS, *row), F32),
            pltpu.VMEM((ROWS, *row), F32),
            pltpu.VMEM((ROWS + 2, *row), F32),
            pltpu.VMEM(row, F32),
            pltpu.VMEM(row, F32),
            pltpu.VMEM((ROWS, *row), F32),
            pltpu.VMEM((ROWS, *row), F32),
            pltpu.VMEM((512, 2048), BF16),
            pltpu.VMEM((512, 1024), BF16),
            pltpu.VMEM((512, 1024), BF16),
            pltpu.VMEM((512, 128), F32),
            pltpu.VMEM((4, MODES, NZ), F32),
            pltpu.VMEM((MODES, NZ), F32),
            pltpu.VMEM((8, PEERS, 8, 128), F32),
            pltpu.VMEM((8, PEERS, 8, 128), F32),
            pltpu.VMEM((ROUNDS, 2, 4, *row), F32),
            pltpu.VMEM((ROUNDS, 2, 4, *row), F32),
            pltpu.VMEM((ROUNDS, 2, *row), F32),
            pltpu.VMEM((ROUNDS, SLABS, *row), F32),
            pltpu.VMEM((4, MODES, NZ), F32),
            pltpu.VMEM((SLABS, 4, MODES, NZ), F32),
            pltpu.VMEM((SLABS, 8, 128), F32),
            pltpu.VMEM((SLABS, 8, 128), F32),
            dma((8,)),
            dma((8,)),
            dma((ROUNDS, 2)),
            dma((ROUNDS, 2)),
            dma((ROUNDS,)),
            dma((ROUNDS,)),
            dma((4,)),
        ],
        compiler_params=pltpu.CompilerParams(
            collective_id=0, has_side_effects=True, vmem_limit_bytes=60 * 1024 * 1024
        ),
        name="channel_adjoint",
    )(
        initial_state,
        drag_rate,
        wall_control,
        lift_profile,
        schur_inverse,
        jnp.asarray(base_table(NX, 1.0 / math.sqrt(NX))),
        jnp.asarray(base_table(NZ, 1.0 / math.sqrt(NZ))),
    )


def solution(mesh):
    return jax.shard_map(
        per_device,
        mesh=mesh,
        in_specs=(
            P(None, None, "gy", "xz", None),
            P("gy", "xz", None),
            P("xz", None),
            P(),
            P("gy", None, "xz", None),
        ),
        out_specs=(P(None, None, "gy", "xz", None), P("xz", "gy")),
        check_vma=False,
    )
```

```python
import functools
import math

import jax
import jax.numpy as jnp
import numpy as np
from jax import lax
from jax.experimental import pallas as pl
from jax.experimental.pallas import tpu as pltpu
from jax.sharding import PartitionSpec as P

MESH = pl.DeviceIdType.MESH
F32 = jnp.float32
BF16 = jnp.bfloat16
DIFFUSION = 0.04
NX = 1024
NZ = 512
KX = 512
ROWS = 8
MODES = 8
PEERS = 64
SLABS = 8
ROUNDS = 4
CONTROL_SLOT = 6
ORDER = (0, 1)


def base_table(period, scale):
    k = np.arange(512)
    high = 2.0 * np.pi * ((32 * np.arange(16)[:, None] * k) % period) / period
    low = 2.0 * np.pi * ((np.arange(32)[:, None] * k) % period) / period
    return np.concatenate(
        [np.cos(high), np.sin(high), np.cos(low) * scale, np.sin(low) * scale]
    ).astype(np.float32)


def split(x):
    hi = x.astype(BF16)
    return hi, (x - hi.astype(F32))


def regrouped(tiles, lane):
    tiles = [pltpu.roll(tiles[-j % 16], 8 * (-j % 16), 1) if j else tiles[0] for j in range(16)]
    for bit in range(4):
        step = 1 << bit
        chosen = (lane // (8 * step)) % 2 == 1
        tiles = [jnp.where(chosen, tiles[(g - step) % 16], tiles[g]) for g in range(16)]
    return [pltpu.roll(tile, 128 - 8 * g, 1) if g else tile for g, tile in enumerate(tiles)]


def kernel(
    state_hbm, drag_hbm, ctrl_hbm, lift_ref, schur_hbm, base_x_hbm, base_z_hbm,
    out_state, out_grad,
    st, pu, pv, pw, divb, direct, pbuf, wall, chat, zin, zout,
    schur, drag_in, ctrl_in, base_x, base_z, txi, tx, tzh, tzl, dg, waves, amat,
    send, recv, hsend, hrecv, ssend, srecv, gsend, grecv, corner, fsend, frecv, csend, crecv,
    send_sem, recv_sem, hsend_sem, hrecv_sem, ssend_sem, srecv_sem, misc_sem, load_sem,
):
    me = lax.axis_index("xz")
    slab = lax.axis_index("gy")
    barrier = pltpu.get_barrier_semaphore()
    loads = [pltpu.make_async_copy(base_z_hbm, base_z, load_sem.at[0])]
    for comp in range(3):
        for c in range(2):
            loads.append(
                pltpu.make_async_copy(
                    state_hbm.at[comp, c],
                    st.at[comp, pl.ds(2, ROWS), c],
                    load_sem.at[1 + 2 * comp + c],
                )
            )
    for k, (source, target) in enumerate(
        ((base_x_hbm, base_x), (drag_hbm, drag_in), (ctrl_hbm, ctrl_in), (schur_hbm, schur))
    ):
        loads.append(pltpu.make_async_copy(source, target, load_sem.at[7 + k]))
    for load in loads:
        load.start()

    @pl.loop(1, PEERS)
    def _(i):
        pl.semaphore_signal(
            barrier, inc=1, device_id=(lax.rem(me + i, PEERS), slab), device_id_type=MESH
        )

    @pl.loop(1, SLABS)
    def _(i):
        pl.semaphore_signal(
            barrier, inc=1, device_id=(me, lax.rem(slab + i, SLABS)), device_id_type=MESH
        )

    lane = lax.broadcasted_iota(jnp.int32, (8, 128), 1)
    wide_lane = lax.broadcasted_iota(jnp.int32, (KX, 128), 1)
    left = wide_lane < 64
    left_half = left[0:256]
    odd_half = lax.broadcasted_iota(jnp.int32, (256, 128), 0) % 2 == 1
    odd = lax.broadcasted_iota(jnp.int32, (KX, 128), 0) % 2 == 1

    mode = me * MODES + lax.broadcasted_iota(jnp.int32, (MODES, NZ), 0)
    span = lax.broadcasted_iota(jnp.int32, (MODES, NZ), 1)
    kx = (2.0 * math.pi / NX) * mode.astype(F32)
    signed = jnp.where(span < NZ // 2, span, span - NZ)
    kz = jnp.where(span == NZ // 2, 0.0, (2.0 * math.pi / NZ) * signed.astype(F32))
    waves[0] = kx
    waves[1] = kz
    waves[2] = kx * kx + kz * kz
    waves[3] = jnp.where(mode == 0, 1.0, 2.0).astype(F32)

    def turns(base, i):
        ca = base[pl.ds(i, 1), :]
        sa = base[pl.ds(16 + i, 1), :]
        cb = base[32:64, :]
        sb = base[64:96, :]
        c_hi, c_lo = split(ca * cb - sa * sb)
        s_hi, s_lo = split(sa * cb + ca * sb)
        return c_hi, c_lo.astype(BF16), s_hi, s_lo.astype(BF16)

    loads[0].wait()

    @pl.loop(0, 16)
    def _(i):
        rows = pl.ds(pl.multiple_of(i * 32, 32), 32)
        tzh[rows, 0:512], tzl[rows, 0:512], tzh[rows, 512:1024], tzl[rows, 512:1024] = turns(
            base_z, i
        )

    def prepare():
        loads[7].wait()

        @pl.loop(0, 16)
        def _(i):
            c_hi, c_lo, s_hi, s_lo = turns(base_x, i)
            rows = pl.ds(pl.multiple_of(i * 32, 32), 32)
            low_rows = pl.ds(pl.multiple_of(512 + i * 32, 32), 32)
            for h in range(2):
                half = slice(256 * h, 256 * h + 256)
                txi[h, rows, 0:256] = c_hi[:, half]
                txi[h, rows, 256:512] = s_hi[:, half]
                txi[h, low_rows, 0:256] = c_lo[:, half]
                txi[h, low_rows, 256:512] = s_lo[:, half]
            for k, part in enumerate((c_hi, c_lo, s_hi, s_lo)):
                start = pl.multiple_of(256 * k + lax.rem(i, 8) * 32, 32)
                tx[i // 8, pl.ds(start, 32)] = part

        loads[8].wait()
        for b in range(4):
            lo = drag_in[:, :, 128 * b : 128 * b + 128].reshape(64, 128)
            hi = drag_in[:, :, 512 + 128 * b : 640 + 128 * b].reshape(64, 128)
            dg[128 * b : 128 * b + 128, :] = jnp.concatenate([lo, hi], axis=0).T

        loads[9].wait()
        for b in range(4):
            near = ctrl_in[:, 128 * b : 128 * b + 128]
            far = ctrl_in[:, 512 + 128 * b : 640 + 128 * b]
            blank = jnp.zeros((56, 128), F32)
            pieces = jnp.concatenate([near, blank, far, blank], axis=0)
            send[CONTROL_SLOT, 16 * b : 16 * b + 16] = pieces.T.reshape(16, 8, 128)
        x_forward(send[CONTROL_SLOT].reshape(KX, 128), CONTROL_SLOT)
        loads[10].wait()
        gsend[0] = schur[0, 7]
        gsend[1] = schur[7, 0]
        gsend[2] = schur[0, 0]
        gsend[3] = schur[7, 7]
        to_slabs(
            lambda peer: gsend.at[pl.ds(0, 3)],
            grecv.at[slab],
            misc_sem.at[0],
            misc_sem.at[1],
        )
        pltpu.make_async_remote_copy(
            src_ref=gsend.at[3],
            dst_ref=corner,
            send_sem=misc_sem.at[4],
            recv_sem=misc_sem.at[5],
            device_id=(me, lax.rem(slab + 1, SLABS)),
            device_id_type=MESH,
        ).start()

    def x_part(value, h):
        hi = value.astype(BF16).astype(F32)
        lo = value - hi
        real = jnp.where(left_half, hi, pltpu.roll(lo, 64, 1))
        imag = -jnp.where(left_half, pltpu.roll(hi, 64, 1), lo)
        rc = jnp.concatenate([real, jnp.where(odd_half, -real, real)], axis=1)
        rs = jnp.concatenate([imag, jnp.where(odd_half, -imag, imag)], axis=1)
        both = jnp.concatenate([rc, rs], axis=0).astype(BF16)
        out = jnp.dot(txi[h], both, preferred_element_type=F32)
        return out[0:KX] + out[KX : 2 * KX]

    def x_folded(out):
        near, far = out[:, 0:128], out[:, 128:256]
        near = near + pltpu.roll(near, 64, 1)
        far = far + pltpu.roll(far, 64, 1)
        return jnp.where(left, near, far)

    def x_inverse(slot):
        out = None
        for hh in ORDER:
            h = (me // 32) ^ hh
            arrived(slot, h, hh == 0)
            part = x_part(recv[slot, pl.ds(h * 32, 32)].reshape(256, 128), h)
            out = part if out is None else out + part
        return x_folded(out)

    def x_forward(value, slot):
        turned = pltpu.roll(value, 64, 1)
        total = value + turned
        gap = jnp.where(left, value - turned, turned - value)

        def packed(part):
            hi = part.astype(BF16).astype(F32)
            return jnp.where(left, hi, part - hi)

        ra = jnp.concatenate([packed(total), packed(gap)], axis=1).astype(BF16)
        def folded(part):
            part = jnp.where(odd_half, part[:, 128:256], part[:, 0:128])
            return part + pltpu.roll(part, 64, 1)

        for hh in (1, 0):
            h = (me // 32) ^ hh
            out = jnp.dot(tx[h], ra, preferred_element_type=F32)
            with_cos = folded(out[0:256] + out[256:512])
            with_sin = folded(out[512:768] + out[768:1024])
            result = jnp.where(left_half, with_cos, -with_sin)
            send[slot, pl.ds(h * 32, 32)] = result.reshape(32, 8, 128)
            exchange(slot, h, hh == 0)

    def z_dot(value, rows):
        count = value.shape[0]
        hi, lo = split(value)
        both = jnp.concatenate([hi, lo.astype(BF16)], axis=0)
        out = jnp.dot(both, tzh[rows, :], preferred_element_type=F32)
        out = out[0:count] + out[count : 2 * count]
        return out + jnp.dot(hi, tzl[rows, :], preferred_element_type=F32)

    def z_inverse(value, slot):
        out = z_dot(value, slice(0, NZ)).reshape(ROWS, 2, MODES, 2 * NZ)
        with_cos, with_sin = out[:, :, :, 0:NZ], out[:, :, :, NZ : 2 * NZ]
        zout[:, 0] = with_cos[:, 0] - with_sin[:, 1]
        zout[:, 1] = with_sin[:, 0] + with_cos[:, 1]

        for hh in (1, 0):
            h = (me // 32) ^ hh
            for j in range(2):
                block = 2 * h + j
                lanes = pl.ds(pl.multiple_of(block * 128, 128), 128)
                tiles = [zout[a % 8, a // 8, :, lanes] for a in range(16)]
                for g, tile in enumerate(regrouped(tiles, lane)):
                    send[slot, block * 16 + g] = tile
            exchange(slot, h, hh == 0)

    def z_forward(slot):
        out = None
        for hh in ORDER:
            h = (me // 32) ^ hh
            arrived(slot, h, hh == 0)
            half = pl.ds(pl.multiple_of(h * 256, 256), 256)
            for j in range(2):
                block = 2 * h + j
                lanes = pl.ds(pl.multiple_of(block * 128, 128), 128)
                tiles = [recv[slot, block * 16 + g] for g in range(16)]
                for a, tile in enumerate(regrouped(tiles, lane)):
                    zin[a % 8, a // 8, :, lanes] = tile
            part = z_dot(zin[:, :, :, half].reshape(128, 256), half)
            out = part if out is None else out + part
        out = out.reshape(ROWS, 2, MODES, 2 * NZ)
        with_cos, with_sin = out[:, :, :, 0:NZ], out[:, :, :, NZ : 2 * NZ]
        zout[:, 0] = with_cos[:, 0] + with_sin[:, 1]
        zout[:, 1] = with_cos[:, 1] - with_sin[:, 0]

    def exchange(slot, h, own):
        for i in range(31, 0 if own else -1, -1):
            peer = h * 32 + (lax.rem(me, 32) ^ i)
            pltpu.make_async_remote_copy(
                src_ref=send.at[slot, peer],
                dst_ref=recv.at[slot, me],
                send_sem=send_sem.at[slot],
                recv_sem=recv_sem.at[slot, me // 32],
                device_id=(peer, slab),
                device_id_type=MESH,
            ).start()
        if own:
            recv[slot, me] = send[slot, me]

    def arrived(slot, h, own):
        whole = recv.at[slot, pl.ds(0, 31 if own else 32)]
        pltpu.make_async_copy(whole, whole, recv_sem.at[slot, h]).wait()

    def left_device(buffer, sem, count):
        whole = buffer.at[pl.ds(0, count)]
        pltpu.make_async_copy(whole, whole, sem).wait()

    def to_slabs(source, target, out_sem, in_sem):
        @pl.loop(1, SLABS)
        def _(i):
            peer = lax.rem(slab + i, SLABS)
            pltpu.make_async_remote_copy(
                src_ref=source(peer),
                dst_ref=target,
                send_sem=out_sem,
                recv_sem=in_sem,
                device_id=(me, peer),
                device_id_type=MESH,
            ).start()

    pl.semaphore_wait(barrier, PEERS - 1 + SLABS - 1)

    loads[1].wait()
    loads[2].wait()
    wall[...] = jnp.zeros_like(wall)

    @pl.loop(0, ROUNDS)
    def _(r):
        adjoint = r // 2
        moving = r != 2
        rate = jnp.where(moving, DIFFUSION, 0.0).astype(F32)

        @pl.when(r == 0)
        def _():
            for load in loads[3:7]:
                load.wait()

        for side, (u_row, v_row) in enumerate(((9, 8), (2, 2))):
            hsend[r, side, 0] = st[0, u_row]
            hsend[r, side, 1] = st[1, v_row]
            hsend[r, side, 2] = st[1, v_row + 1]
            hsend[r, side, 3] = st[2, u_row]
        def send_halo(part):
            for side in range(2):
                rows = part(side)
                pltpu.make_async_remote_copy(
                    src_ref=hsend.at[r, side, rows],
                    dst_ref=hrecv.at[r, side, rows],
                    send_sem=hsend_sem.at[r, side],
                    recv_sem=hrecv_sem.at[r, side],
                    device_id=(me, lax.rem(slab + (1 if side == 0 else SLABS - 1), SLABS)),
                    device_id_type=MESH,
                ).start()

        def wait_halo(part, buffer, sem):
            for side in range(2):
                whole = buffer.at[r, side, part(side)]
                pltpu.make_async_copy(whole, whole, sem.at[r, side]).wait()

        def all_rows(side):
            return pl.ds(0, 4)

        def near_row(side):
            return pl.ds(2 - side, 1)

        @pl.when(moving)
        def _():
            send_halo(all_rows)

        @pl.when(r == 2)
        def _():
            send_halo(near_row)

        @pl.when(moving)
        def _():
            before = jnp.where(r < 2, waves[3], 1.0)
            z_inverse((st[0, 2:10] * before).reshape(128, NZ), 2 * jnp.where(r == 3, 2, r))

        @pl.when(r == 0)
        def _():
            prepare()

        @pl.when(moving)
        def _():
            wait_halo(all_rows, hrecv, hrecv_sem)
            for side, (u_row, v_row, edge) in enumerate(((1, 0, 0), (10, 10, SLABS - 1))):
                open_side = slab != edge
                st[0, u_row] = jnp.where(open_side, hrecv[r, side, 0], 0.0)
                st[1, v_row] = jnp.where(open_side, hrecv[r, side, 1], 0.0)
                st[1, v_row + 1] = jnp.where(open_side, hrecv[r, side, 2], 0.0)
                st[2, u_row] = jnp.where(open_side, hrecv[r, side, 3], 0.0)

        @pl.when(r == 2)
        def _():
            wait_halo(near_row, hrecv, hrecv_sem)
            for side, (v_row, edge) in enumerate(((1, 0), (10, SLABS - 1))):
                st[1, v_row] = jnp.where(slab != edge, hrecv[r, side, 2 - side], 0.0)

        square = waves[2]

        def diffused(comp, row):
            middle = st[comp, row]
            around = st[comp, row + 1] - 2.0 * middle + st[comp, row - 1]
            return middle + rate * (around - square * middle)

        @pl.loop(0, ROWS)
        def _(y):
            pu[y] = diffused(0, y + 2)
            pw[y] = diffused(2, y + 2)

        @pl.loop(0, ROWS + 2)
        def _(y):
            row = slab * ROWS + y - 1
            inside = jnp.logical_and(row >= 0, row < ROWS * SLABS)
            pv[y] = jnp.where(inside, diffused(1, y + 1), 0.0)

        @pl.when(moving)
        def _():
            slot = 2 * jnp.where(r == 3, 2, r)
            x_forward(x_inverse(slot) * dg[...], slot + 1)

        @pl.when(r == 0)
        def _():
            z_forward(CONTROL_SLOT)
            chat[...] = zout[0]
            pltpu.make_async_copy(
                grecv.at[pl.ds(0, SLABS - 1)], grecv.at[pl.ds(0, SLABS - 1)], misc_sem.at[1]
            ).wait()
            pltpu.make_async_copy(corner, corner, misc_sem.at[5]).wait()

            def gather_a(i, a):
                b = SLABS - 1 - i
                return grecv[b, 2] + grecv[b, 0] * a * grecv[b, 1]

            amat[...] = lax.fori_loop(0, SLABS - 1 - slab, gather_a, jnp.zeros((MODES, NZ), F32))

        @pl.when(r < 2)
        def _():
            @pl.loop(0, ROWS + 2)
            def _(y):
                row = slab * ROWS + y - 1
                inside = jnp.logical_and(row >= 0, row < ROWS * SLABS)
                safe = jnp.clip(row, 0, ROWS * SLABS - 1)
                level = jnp.where(inside, lift_ref[safe], 0.0)
                pv[y] = pv[y] + level * chat[...]

        kxv, kzv = waves[0], waves[1]

        @pl.when(moving)
        def _():
            slot = 2 * jnp.where(r == 3, 2, r) + 1
            z_forward(slot)
            after = jnp.where(r < 2, 1.0, waves[3])

            @pl.loop(0, ROWS)
            def _(y):
                pu[y] = pu[y] - zout[y] * after

        @pl.loop(0, ROWS)
        def _(y):
            slope = 0.5 * (pv[y + 2] - pv[y])
            divb[y, 0] = slope[0] - kxv * pu[y, 1] - kzv * pw[y, 1]
            divb[y, 1] = slope[1] + kxv * pu[y, 0] + kzv * pw[y, 0]

        def entry(i, j):
            return schur[i + adjoint * (j - i), j + adjoint * (i - j)]

        def solve_row(i):
            total = entry(i, 0) * divb[0]
            for j in range(1, ROWS):
                total = total + entry(i, j) * divb[j]
            direct[i] = total

        @pl.loop(0, 2)
        def _(i):
            solve_row(7 * i)

        ratio = entry(7, 0)
        turn = entry(0, 7)
        last = direct[7]
        ssend[r, 0] = last
        ssend[r, 1] = direct[0] + turn * (amat[...] * last)
        to_slabs(
            lambda peer: ssend.at[r, jnp.where(peer > slab, 0, 1)],
            srecv.at[r, slab],
            ssend_sem.at[r],
            srecv_sem.at[r],
        )

        @pl.loop(1, ROWS - 1)
        def _(i):
            solve_row(i)

        whole = srecv.at[r, pl.ds(0, SLABS - 1)]
        pltpu.make_async_copy(whole, whole, srecv_sem.at[r]).wait()

        blank = jnp.zeros((2, MODES, NZ), F32)
        entering = lax.fori_loop(
            0, slab, lambda b, z: srecv[r, b] + grecv[b, 1 - adjoint] * z, blank
        )

        def suffix(i, e):
            b = SLABS - 1 - i
            return srecv[r, b] + grecv[b, adjoint] * e

        above = lax.fori_loop(0, SLABS - 1 - slab, suffix, blank)
        leaving = above + amat[...] * (last + ratio * entering)
        pbuf[9] = leaving

        @pl.loop(0, ROWS)
        def _(i):
            pbuf[i + 1] = direct[i] + entry(i, 0) * entering + entry(i, 7) * leaving

        pbuf[0] = jnp.where(slab == 0, 0.0, entering + corner[...] * pbuf[1])

        @pl.loop(0, ROWS)
        def _(y):
            p0, p1 = pbuf[y + 1, 0], pbuf[y + 1, 1]
            st[0, y + 2, 0] = pu[y, 0] + kxv * p1
            st[0, y + 2, 1] = pu[y, 1] - kxv * p0
            st[2, y + 2, 0] = pw[y, 0] + kzv * p1
            st[2, y + 2, 1] = pw[y, 1] - kzv * p0
            normal = pv[y + 1] - 0.5 * (pbuf[y + 2] - pbuf[y])
            st[1, y + 2] = normal
            level = jnp.where(r >= 2, lift_ref[slab * ROWS + y], 0.0)
            wall[...] = wall[...] + level * normal

        @pl.when(r == 1)
        def _():
            @pl.loop(0, ROWS)
            def _(y):
                for comp in range(3):
                    for c in range(2):
                        out_state[comp, c, y] = st[comp, y + 2, c]

    out = z_dot(wall[...].reshape(16, NZ), slice(0, NZ))
    rows16 = jnp.concatenate(
        [out[0:8, 0:NZ] - out[8:16, NZ:], out[0:8, NZ:] + out[8:16, 0:NZ]], axis=0
    )
    row16 = lax.broadcasted_iota(jnp.int32, (16, 128), 0)
    lane16 = lax.broadcasted_iota(jnp.int32, (16, 128), 1) // 8
    for block in range(4):
        piece = rows16[:, 128 * block : 128 * block + 128]
        for bit in range(4):
            step = 1 << bit
            piece = jnp.where(
                (row16 // step) % 2 == 1, pltpu.roll(piece, 128 - 8 * step, 1), piece
            )
        for bit in range(4):
            step = 1 << bit
            piece = jnp.where((lane16 // step) % 2 == 1, pltpu.roll(piece, step, 0), piece)
        for g in range(16):
            csend[16 * block + g] = piece[g : g + 1]

    for i in range(PEERS - 1, 0, -1):
        peer = me ^ i
        pltpu.make_async_remote_copy(
            src_ref=csend.at[peer],
            dst_ref=crecv.at[me],
            send_sem=misc_sem.at[6],
            recv_sem=misc_sem.at[7],
            device_id=(peer, slab),
            device_id_type=MESH,
        ).start()
    crecv[me] = csend[me]
    left_device(crecv, misc_sem.at[7], PEERS - 1)
    plane = jnp.broadcast_to(crecv[...], (PEERS, 8, 128)).reshape(KX, 128)
    plane = pltpu.roll(plane, lax.rem(128 - 8 * lax.rem(me, 16), 128), 1)
    rank = lax.broadcasted_iota(jnp.int32, (KX, 128), 0)
    for bit in range(3):
        step = 1 << bit
        plane = jnp.where((rank // step) % 2 == 1, pltpu.roll(plane, 8 * step, 1), plane)
    plane = x_folded(x_part(plane[0:256], 0) + x_part(plane[256:512], 1))
    for b in range(4):
        turned = plane[128 * b : 128 * b + 128, :].T
        fsend[b] = turned[0:8]
        fsend[4 + b] = turned[64:72]
    to_slabs(
        lambda peer: fsend.at[peer], frecv.at[slab], misc_sem.at[2], misc_sem.at[3]
    )
    frecv[slab] = fsend[slab]
    left_device(frecv, misc_sem.at[3], SLABS - 1)
    total = frecv[0]
    for b in range(1, SLABS):
        total = total + frecv[b]
    out_grad[...] = total

    @pl.loop(0, 7)
    def _(slot):
        left_device(send.at[slot], send_sem.at[slot], PEERS - 1)

    @pl.loop(0, ROUNDS)
    def _(r):
        left_device(srecv.at[r], ssend_sem.at[r], SLABS - 1)
        for side in range(2):
            @pl.when(r != 2)
            def _():
                whole = hsend.at[r, side]
                pltpu.make_async_copy(whole, whole, hsend_sem.at[r, side]).wait()

            @pl.when(r == 2)
            def _():
                whole = hsend.at[r, side, pl.ds(0, 1)]
                pltpu.make_async_copy(whole, whole, hsend_sem.at[r, side]).wait()

    left_device(grecv, misc_sem.at[0], SLABS - 1)
    pltpu.make_async_copy(corner, corner, misc_sem.at[4]).wait()
    left_device(frecv, misc_sem.at[2], SLABS - 1)
    left_device(crecv, misc_sem.at[6], PEERS - 1)


def per_device(initial_state, drag_rate, wall_control, lift_profile, schur_inverse):
    row = (2, MODES, NZ)
    vmem = pl.BlockSpec(memory_space=pltpu.VMEM)
    hbm = pl.BlockSpec(memory_space=pl.ANY)
    smem = pl.BlockSpec(memory_space=pltpu.SMEM)
    dma = pltpu.SemaphoreType.DMA
    return pl.pallas_call(
        kernel,
        out_shape=(
            jax.ShapeDtypeStruct((3, 2, ROWS, MODES, NZ), F32),
            jax.ShapeDtypeStruct((8, 128), F32),
        ),
        in_specs=[hbm, hbm, hbm, smem, hbm, hbm, hbm],
        out_specs=(vmem, vmem),
        scratch_shapes=[
            pltpu.VMEM((3, ROWS + 4, *row), F32),
            pltpu.VMEM((ROWS, *row), F32),
            pltpu.VMEM((ROWS + 2, *row), F32),
            pltpu.VMEM((ROWS, *row), F32),
            pltpu.VMEM((ROWS, *row), F32),
            pltpu.VMEM((ROWS, *row), F32),
            pltpu.VMEM((ROWS + 2, *row), F32),
            pltpu.VMEM(row, F32),
            pltpu.VMEM(row, F32),
            pltpu.VMEM((ROWS, *row), F32),
            pltpu.VMEM((ROWS, *row), F32),
            pltpu.VMEM((ROWS, ROWS, MODES, NZ), F32),
            pltpu.VMEM((ROWS, MODES, NX), F32),
            pltpu.VMEM((8, NX), F32),
            pltpu.VMEM((96, 512), F32),
            pltpu.VMEM((96, 512), F32),
            pltpu.VMEM((2, 1024, 512), BF16),
            pltpu.VMEM((2, 1024, 512), BF16),
            pltpu.VMEM((512, 1024), BF16),
            pltpu.VMEM((512, 1024), BF16),
            pltpu.VMEM((512, 128), F32),
            pltpu.VMEM((4, MODES, NZ), F32),
            pltpu.VMEM((MODES, NZ), F32),
            pltpu.VMEM((7, PEERS, 8, 128), F32),
            pltpu.VMEM((7, PEERS, 8, 128), F32),
            pltpu.VMEM((ROUNDS, 2, 4, *row), F32),
            pltpu.VMEM((ROUNDS, 2, 4, *row), F32),
            pltpu.VMEM((ROUNDS, 2, *row), F32),
            pltpu.VMEM((ROUNDS, SLABS, *row), F32),
            pltpu.VMEM((4, MODES, NZ), F32),
            pltpu.VMEM((SLABS, 3, MODES, NZ), F32),
            pltpu.VMEM((MODES, NZ), F32),
            pltpu.VMEM((SLABS, 8, 128), F32),
            pltpu.VMEM((SLABS, 8, 128), F32),
            pltpu.VMEM((PEERS, 1, 128), F32),
            pltpu.VMEM((PEERS, 1, 128), F32),
            dma((7,)),
            dma((7, 2)),
            dma((ROUNDS, 2)),
            dma((ROUNDS, 2)),
            dma((ROUNDS,)),
            dma((ROUNDS,)),
            dma((8,)),
            dma((11,)),
        ],
        compiler_params=pltpu.CompilerParams(
            collective_id=0, has_side_effects=True, vmem_limit_bytes=60 * 1024 * 1024
        ),
        name="channel_adjoint",
    )(
        initial_state,
        drag_rate,
        wall_control,
        lift_profile,
        schur_inverse,
        jnp.asarray(base_table(NX, 1.0 / math.sqrt(NX))),
        jnp.asarray(base_table(NZ, 1.0 / math.sqrt(NZ))),
    )


def solution(mesh):
    return jax.shard_map(
        per_device,
        mesh=mesh,
        in_specs=(
            P(None, None, "gy", "xz", None),
            P("gy", "xz", None),
            P("xz", None),
            P(),
            P("gy", None, "xz", None),
        ),
        out_specs=(P(None, None, "gy", "xz", None), P("xz", "gy")),
        check_vma=False,
    )
```

```python
import functools
import math

import jax
import jax.numpy as jnp
import numpy as np
from jax import lax
from jax.experimental import pallas as pl
from jax.experimental.pallas import tpu as pltpu
from jax.sharding import PartitionSpec as P

MESH = pl.DeviceIdType.MESH
F32 = jnp.float32
BF16 = jnp.bfloat16
DIFFUSION = 0.04
NX = 1024
NZ = 512
KX = 512
ROWS = 8
MODES = 8
PEERS = 64
SLABS = 8
ROUNDS = 4
CONTROL_SLOT = 6
ORDER = (0, 1)


def base_table(period, scale):
    k = np.arange(512)
    high = 2.0 * np.pi * ((32 * np.arange(16)[:, None] * k) % period) / period
    low = 2.0 * np.pi * ((np.arange(32)[:, None] * k) % period) / period
    return np.concatenate(
        [np.cos(high), np.sin(high), np.cos(low) * scale, np.sin(low) * scale]
    ).astype(np.float32)


def split(x):
    hi = x.astype(BF16)
    return hi, (x - hi.astype(F32))


def regrouped(tiles, lane):
    tiles = [pltpu.roll(tiles[-j % 16], 8 * (-j % 16), 1) if j else tiles[0] for j in range(16)]
    for bit in range(4):
        step = 1 << bit
        chosen = (lane // (8 * step)) % 2 == 1
        tiles = [jnp.where(chosen, tiles[(g - step) % 16], tiles[g]) for g in range(16)]
    return [pltpu.roll(tile, 128 - 8 * g, 1) if g else tile for g, tile in enumerate(tiles)]


def kernel(
    state_hbm, drag_hbm, ctrl_hbm, lift_ref, schur_hbm, base_x_hbm, base_z_hbm,
    out_state, out_grad,
    st, pu, pv, pw, divb, direct, pbuf, wall, chat, zin, zout,
    schur, drag_in, ctrl_in, base_x, base_z, txi, tx, tzh, tzl, dg, waves, amat,
    send, recv, hsend, hrecv, ssend, srecv, gsend, grecv, corner, fsend, frecv, csend, crecv,
    send_sem, recv_sem, hsend_sem, hrecv_sem, ssend_sem, srecv_sem, misc_sem, load_sem,
):
    me = lax.axis_index("xz")
    slab = lax.axis_index("gy")
    barrier = pltpu.get_barrier_semaphore()
    loads = [pltpu.make_async_copy(base_z_hbm, base_z, load_sem.at[0])]
    for comp in range(3):
        for c in range(2):
            loads.append(
                pltpu.make_async_copy(
                    state_hbm.at[comp, c],
                    st.at[comp, pl.ds(2, ROWS), c],
                    load_sem.at[1 + 2 * comp + c],
                )
            )
    for k, (source, target) in enumerate(
        ((base_x_hbm, base_x), (drag_hbm, drag_in), (ctrl_hbm, ctrl_in), (schur_hbm, schur))
    ):
        loads.append(pltpu.make_async_copy(source, target, load_sem.at[7 + k]))
    for load in loads:
        load.start()
    stores = [
        pltpu.make_async_copy(
            st.at[comp, pl.ds(2, ROWS), c],
            out_state.at[comp, c],
            load_sem.at[11 + 2 * comp + c],
        )
        for comp in range(3)
        for c in range(2)
    ]

    @pl.loop(1, PEERS)
    def _(i):
        pl.semaphore_signal(
            barrier, inc=1, device_id=(lax.rem(me + i, PEERS), slab), device_id_type=MESH
        )

    @pl.loop(1, SLABS)
    def _(i):
        pl.semaphore_signal(
            barrier, inc=1, device_id=(me, lax.rem(slab + i, SLABS)), device_id_type=MESH
        )

    lane = lax.broadcasted_iota(jnp.int32, (8, 128), 1)
    wide_lane = lax.broadcasted_iota(jnp.int32, (KX, 128), 1)
    left = wide_lane < 64
    left_half = left[0:256]
    odd_half = lax.broadcasted_iota(jnp.int32, (256, 128), 0) % 2 == 1
    odd = lax.broadcasted_iota(jnp.int32, (KX, 128), 0) % 2 == 1

    mode = me * MODES + lax.broadcasted_iota(jnp.int32, (MODES, NZ), 0)
    span = lax.broadcasted_iota(jnp.int32, (MODES, NZ), 1)
    kx = (2.0 * math.pi / NX) * mode.astype(F32)
    signed = jnp.where(span < NZ // 2, span, span - NZ)
    kz = jnp.where(span == NZ // 2, 0.0, (2.0 * math.pi / NZ) * signed.astype(F32))
    waves[0] = kx
    waves[1] = kz
    waves[2] = kx * kx + kz * kz
    waves[3] = jnp.where(mode == 0, 1.0, 2.0).astype(F32)

    def turns(base, i):
        ca = base[pl.ds(i, 1), :]
        sa = base[pl.ds(16 + i, 1), :]
        cb = base[32:64, :]
        sb = base[64:96, :]
        c_hi, c_lo = split(ca * cb - sa * sb)
        s_hi, s_lo = split(sa * cb + ca * sb)
        return c_hi, c_lo.astype(BF16), s_hi, s_lo.astype(BF16)

    loads[0].wait()

    @pl.loop(0, 16)
    def _(i):
        rows = pl.ds(pl.multiple_of(i * 32, 32), 32)
        tzh[rows, 0:512], tzl[rows, 0:512], tzh[rows, 512:1024], tzl[rows, 512:1024] = turns(
            base_z, i
        )

    def prepare():
        loads[7].wait()

        @pl.loop(0, 16)
        def _(i):
            c_hi, c_lo, s_hi, s_lo = turns(base_x, i)
            rows = pl.ds(pl.multiple_of(i * 32, 32), 32)
            low_rows = pl.ds(pl.multiple_of(512 + i * 32, 32), 32)
            txi[rows, 0:512] = c_hi
            txi[rows, 512:1024] = s_hi
            txi[low_rows, 0:512] = c_lo
            txi[low_rows, 512:1024] = s_lo
            for k, part in enumerate((c_hi, c_lo, s_hi, s_lo)):
                start = pl.multiple_of(256 * k + lax.rem(i, 8) * 32, 32)
                tx[i // 8, pl.ds(start, 32)] = part

        loads[8].wait()
        for b in range(4):
            lo = drag_in[:, :, 128 * b : 128 * b + 128].reshape(64, 128)
            hi = drag_in[:, :, 512 + 128 * b : 640 + 128 * b].reshape(64, 128)
            dg[128 * b : 128 * b + 128, :] = jnp.concatenate([lo, hi], axis=0).T

        loads[9].wait()
        for b in range(4):
            near = ctrl_in[:, 128 * b : 128 * b + 128]
            far = ctrl_in[:, 512 + 128 * b : 640 + 128 * b]
            blank = jnp.zeros((56, 128), F32)
            pieces = jnp.concatenate([near, blank, far, blank], axis=0)
            send[CONTROL_SLOT, 16 * b : 16 * b + 16] = pieces.T.reshape(16, 8, 128)
        x_forward(send[CONTROL_SLOT].reshape(KX, 128), CONTROL_SLOT)
        loads[10].wait()
        gsend[0] = schur[0, 7]
        gsend[1] = schur[7, 0]
        gsend[2] = schur[0, 0]
        gsend[3] = schur[7, 7]
        to_slabs(
            lambda peer: gsend.at[pl.ds(0, 3)],
            grecv.at[slab],
            misc_sem.at[0],
            misc_sem.at[1],
        )
        pltpu.make_async_remote_copy(
            src_ref=gsend.at[3],
            dst_ref=corner,
            send_sem=misc_sem.at[4],
            recv_sem=misc_sem.at[5],
            device_id=(me, lax.rem(slab + 1, SLABS)),
            device_id_type=MESH,
        ).start()

    def x_part(value):
        hi = value.astype(BF16).astype(F32)
        lo = value - hi
        real = jnp.where(left, hi, pltpu.roll(lo, 64, 1))
        imag = -jnp.where(left, pltpu.roll(hi, 64, 1), lo)
        rc = jnp.concatenate([real, jnp.where(odd, -real, real)], axis=1)
        rs = jnp.concatenate([imag, jnp.where(odd, -imag, imag)], axis=1)
        both = jnp.concatenate([rc, rs], axis=0).astype(BF16)
        out = jnp.dot(txi[...], both, preferred_element_type=F32)
        out = out[0:KX] + out[KX : 2 * KX]
        near, far = out[:, 0:128], out[:, 128:256]
        near = near + pltpu.roll(near, 64, 1)
        far = far + pltpu.roll(far, 64, 1)
        return jnp.where(left, near, far)

    def x_inverse(slot):
        for hh in ORDER:
            arrived(slot, (me // 32) ^ hh, hh == 0)
        return x_part(recv[slot].reshape(KX, 128))

    def x_forward(value, slot):
        turned = pltpu.roll(value, 64, 1)
        total = value + turned
        gap = jnp.where(left, value - turned, turned - value)

        def packed(part):
            hi = part.astype(BF16).astype(F32)
            return jnp.where(left, hi, part - hi)

        ra = jnp.concatenate([packed(total), packed(gap)], axis=1).astype(BF16)
        def folded(part):
            part = jnp.where(odd_half, part[:, 128:256], part[:, 0:128])
            return part + pltpu.roll(part, 64, 1)

        for hh in (1, 0):
            h = (me // 32) ^ hh
            out = jnp.dot(tx[h], ra, preferred_element_type=F32)
            with_cos = folded(out[0:256] + out[256:512])
            with_sin = folded(out[512:768] + out[768:1024])
            result = jnp.where(left_half, with_cos, -with_sin)
            send[slot, pl.ds(h * 32, 32)] = result.reshape(32, 8, 128)
            exchange(slot, h, hh == 0)

    def z_dot(value, rows):
        count = value.shape[0]
        hi, lo = split(value)
        both = jnp.concatenate([hi, lo.astype(BF16)], axis=0)
        out = jnp.dot(both, tzh[rows, :], preferred_element_type=F32)
        out = out[0:count] + out[count : 2 * count]
        return out + jnp.dot(hi, tzl[rows, :], preferred_element_type=F32)

    def z_inverse(value, slot, sent):
        out = z_dot(value, slice(0, NZ)).reshape(ROWS, 2, MODES, 2 * NZ)
        with_cos, with_sin = out[:, :, :, 0:NZ], out[:, :, :, NZ : 2 * NZ]
        zout[:, 0] = with_cos[:, 0] - with_sin[:, 1]
        zout[:, 1] = with_sin[:, 0] + with_cos[:, 1]

        for hh in (1, 0):
            h = (me // 32) ^ hh
            for j in range(2):
                block = 2 * h + j
                lanes = pl.ds(pl.multiple_of(block * 128, 128), 128)
                tiles = [zout[a % 8, a // 8, :, lanes] for a in range(16)]
                for g, tile in enumerate(regrouped(tiles, lane)):
                    send[slot, block * 16 + g] = tile
            if sent:
                exchange(slot, h, hh == 0)

    def z_forward(slot):
        out = None
        for hh in ORDER:
            h = (me // 32) ^ hh
            arrived(slot, h, hh == 0)
            half = pl.ds(pl.multiple_of(h * 256, 256), 256)
            for j in range(2):
                block = 2 * h + j
                lanes = pl.ds(pl.multiple_of(block * 128, 128), 128)
                tiles = [recv[slot, block * 16 + g] for g in range(16)]
                for a, tile in enumerate(regrouped(tiles, lane)):
                    zin[a % 8, a // 8, :, lanes] = tile
            part = z_dot(zin[:, :, :, half].reshape(128, 256), half)
            out = part if out is None else out + part
        out = out.reshape(ROWS, 2, MODES, 2 * NZ)
        with_cos, with_sin = out[:, :, :, 0:NZ], out[:, :, :, NZ : 2 * NZ]
        zout[:, 0] = with_cos[:, 0] + with_sin[:, 1]
        zout[:, 1] = with_cos[:, 1] - with_sin[:, 0]

    def exchange(slot, h, own):
        order = [8 * y + x for x in range(8) for y in range(4)][::-1]
        for i in [k for k in order if k or not own]:
            peer = h * 32 + (lax.rem(me, 32) ^ i)
            pltpu.make_async_remote_copy(
                src_ref=send.at[slot, peer],
                dst_ref=recv.at[slot, me],
                send_sem=send_sem.at[slot],
                recv_sem=recv_sem.at[slot, me // 32],
                device_id=(peer, slab),
                device_id_type=MESH,
            ).start()
        if own:
            recv[slot, me] = send[slot, me]

    def arrived(slot, h, own):
        whole = recv.at[slot, pl.ds(0, 31 if own else 32)]
        pltpu.make_async_copy(whole, whole, recv_sem.at[slot, h]).wait()

    def left_device(buffer, sem, count):
        whole = buffer.at[pl.ds(0, count)]
        pltpu.make_async_copy(whole, whole, sem).wait()

    def to_slabs(source, target, out_sem, in_sem):
        for i in (4, 3, 5, 2, 6, 1, 7):
            peer = lax.rem(slab + i, SLABS)
            pltpu.make_async_remote_copy(
                src_ref=source(peer),
                dst_ref=target,
                send_sem=out_sem,
                recv_sem=in_sem,
                device_id=(me, peer),
                device_id_type=MESH,
            ).start()

    loads[1].wait()
    loads[2].wait()
    z_inverse((st[0, 2:10] * waves[3]).reshape(128, NZ), 0, False)
    pl.semaphore_wait(barrier, PEERS - 1 + SLABS - 1)
    for hh in (1, 0):
        exchange(0, (me // 32) ^ hh, hh == 0)
    wall[...] = jnp.zeros_like(wall)

    @pl.loop(0, ROUNDS)
    def _(r):
        adjoint = r // 2
        moving = r != 2
        rate = jnp.where(moving, DIFFUSION, 0.0).astype(F32)

        @pl.when(r == 0)
        def _():
            for load in loads[3:7]:
                load.wait()

        for side, (u_row, v_row) in enumerate(((9, 8), (2, 2))):
            hsend[r, side, 0] = st[0, u_row]
            hsend[r, side, 1] = st[1, v_row]
            hsend[r, side, 2] = st[1, v_row + 1]
            hsend[r, side, 3] = st[2, u_row]
        def send_halo(part):
            for side in range(2):
                rows = part(side)
                pltpu.make_async_remote_copy(
                    src_ref=hsend.at[r, side, rows],
                    dst_ref=hrecv.at[r, side, rows],
                    send_sem=hsend_sem.at[r, side],
                    recv_sem=hrecv_sem.at[r, side],
                    device_id=(me, lax.rem(slab + (1 if side == 0 else SLABS - 1), SLABS)),
                    device_id_type=MESH,
                ).start()

        def wait_halo(part, buffer, sem):
            for side in range(2):
                whole = buffer.at[r, side, part(side)]
                pltpu.make_async_copy(whole, whole, sem.at[r, side]).wait()

        def all_rows(side):
            return pl.ds(0, 4)

        def near_row(side):
            return pl.ds(2 - side, 1)

        @pl.when(moving)
        def _():
            send_halo(all_rows)

        @pl.when(r == 2)
        def _():
            send_halo(near_row)

        @pl.when(jnp.logical_or(r == 1, r == 3))
        def _():
            before = jnp.where(r < 2, waves[3], 1.0)
            value = (st[0, 2:10] * before).reshape(128, NZ)
            z_inverse(value, 2 * jnp.where(r == 3, 2, r), True)

        @pl.when(r == 0)
        def _():
            prepare()

        @pl.when(moving)
        def _():
            wait_halo(all_rows, hrecv, hrecv_sem)
            for side, (u_row, v_row, edge) in enumerate(((1, 0, 0), (10, 10, SLABS - 1))):
                open_side = slab != edge
                st[0, u_row] = jnp.where(open_side, hrecv[r, side, 0], 0.0)
                st[1, v_row] = jnp.where(open_side, hrecv[r, side, 1], 0.0)
                st[1, v_row + 1] = jnp.where(open_side, hrecv[r, side, 2], 0.0)
                st[2, u_row] = jnp.where(open_side, hrecv[r, side, 3], 0.0)

        @pl.when(r == 2)
        def _():
            st[1, 1] = jnp.zeros((2, MODES, NZ), F32)
            st[1, 10] = jnp.zeros((2, MODES, NZ), F32)

        square = waves[2]

        def diffused(comp, row):
            middle = st[comp, row]
            around = st[comp, row + 1] - 2.0 * middle + st[comp, row - 1]
            return middle + rate * (around - square * middle)

        @pl.loop(0, ROWS)
        def _(y):
            pu[y] = diffused(0, y + 2)
            pw[y] = diffused(2, y + 2)

        @pl.loop(0, ROWS + 2)
        def _(y):
            row = slab * ROWS + y - 1
            inside = jnp.logical_and(row >= 0, row < ROWS * SLABS)
            pv[y] = jnp.where(inside, diffused(1, y + 1), 0.0)

        @pl.when(moving)
        def _():
            slot = 2 * jnp.where(r == 3, 2, r)
            x_forward(x_inverse(slot) * dg[...], slot + 1)

        @pl.when(r == 0)
        def _():
            z_forward(CONTROL_SLOT)
            chat[...] = zout[0]
            pltpu.make_async_copy(
                grecv.at[pl.ds(0, SLABS - 1)], grecv.at[pl.ds(0, SLABS - 1)], misc_sem.at[1]
            ).wait()
            pltpu.make_async_copy(corner, corner, misc_sem.at[5]).wait()

            def gather_a(i, a):
                b = SLABS - 1 - i
                return grecv[b, 2] + grecv[b, 0] * a * grecv[b, 1]

            amat[...] = lax.fori_loop(0, SLABS - 1 - slab, gather_a, jnp.zeros((MODES, NZ), F32))

        @pl.when(r < 2)
        def _():
            @pl.loop(0, ROWS + 2)
            def _(y):
                row = slab * ROWS + y - 1
                inside = jnp.logical_and(row >= 0, row < ROWS * SLABS)
                safe = jnp.clip(row, 0, ROWS * SLABS - 1)
                level = jnp.where(inside, lift_ref[safe], 0.0)
                pv[y] = pv[y] + level * chat[...]

        kxv, kzv = waves[0], waves[1]

        @pl.when(moving)
        def _():
            slot = 2 * jnp.where(r == 3, 2, r) + 1
            z_forward(slot)
            after = jnp.where(r < 2, 1.0, waves[3])

            @pl.loop(0, ROWS)
            def _(y):
                pu[y] = pu[y] - zout[y] * after

        @pl.loop(0, ROWS)
        def _(y):
            slope = 0.5 * (pv[y + 2] - pv[y])
            divb[y, 0] = slope[0] - kxv * pu[y, 1] - kzv * pw[y, 1]
            divb[y, 1] = slope[1] + kxv * pu[y, 0] + kzv * pw[y, 0]

        def entry(i, j):
            return schur[i + adjoint * (j - i), j + adjoint * (i - j)]

        def solve_row(i):
            total = entry(i, 0) * divb[0]
            for j in range(1, ROWS):
                total = total + entry(i, j) * divb[j]
            direct[i] = total

        @pl.loop(0, 2)
        def _(i):
            solve_row(7 * i)

        ratio = entry(7, 0)
        turn = entry(0, 7)
        half = jnp.where(r == 2, 0.5, 0.0).astype(F32)
        last = direct[7] - half * st[1, 9]
        first_v = half * st[1, 2]
        cross = jnp.where(slab == 0, 0.0, corner[...] * first_v)
        ssend[r, 0] = last + ratio * cross
        ssend[r, 1] = (
            direct[0]
            + turn * (amat[...] * last)
            + first_v
            + (schur[0, 0] + turn * amat[...] * ratio) * cross
        )
        to_slabs(
            lambda peer: ssend.at[r, jnp.where(peer > slab, 0, 1)],
            srecv.at[r, slab],
            ssend_sem.at[r],
            srecv_sem.at[r],
        )

        @pl.loop(1, ROWS - 1)
        def _(i):
            solve_row(i)

        whole = srecv.at[r, pl.ds(0, SLABS - 1)]
        pltpu.make_async_copy(whole, whole, srecv_sem.at[r]).wait()

        blank = jnp.zeros((2, MODES, NZ), F32)
        entering = lax.fori_loop(
            0, slab, lambda b, z: srecv[r, b] + grecv[b, 1 - adjoint] * z, blank
        )
        entering = entering + cross

        def suffix(i, e):
            b = SLABS - 1 - i
            return srecv[r, b] + grecv[b, adjoint] * e

        above = lax.fori_loop(0, SLABS - 1 - slab, suffix, blank)
        leaving = above + amat[...] * (last + ratio * entering)
        pbuf[9] = leaving

        @pl.loop(0, ROWS)
        def _(i):
            pbuf[i + 1] = direct[i] + entry(i, 0) * entering + entry(i, 7) * leaving

        pbuf[0] = jnp.where(slab == 0, 0.0, entering + corner[...] * pbuf[1])

        @pl.when(r == 2)
        def _():
            wait_halo(near_row, hrecv, hrecv_sem)
            pbuf[0] = pbuf[0] + jnp.where(slab == 0, 0.0, 0.5 * hrecv[r, 0, 2])
            pbuf[9] = pbuf[9] - jnp.where(slab == SLABS - 1, 0.0, 0.5 * hrecv[r, 1, 1])
            for copy in stores:
                copy.wait()

        @pl.loop(0, ROWS)
        def _(y):
            p0, p1 = pbuf[y + 1, 0], pbuf[y + 1, 1]
            st[0, y + 2, 0] = pu[y, 0] + kxv * p1
            st[0, y + 2, 1] = pu[y, 1] - kxv * p0
            st[2, y + 2, 0] = pw[y, 0] + kzv * p1
            st[2, y + 2, 1] = pw[y, 1] - kzv * p0
            normal = pv[y + 1] - 0.5 * (pbuf[y + 2] - pbuf[y])
            st[1, y + 2] = normal
            level = jnp.where(r >= 2, lift_ref[slab * ROWS + y], 0.0)
            wall[...] = wall[...] + level * normal

        @pl.when(r == 1)
        def _():
            for copy in stores:
                copy.start()

    out = z_dot(wall[...].reshape(16, NZ), slice(0, NZ))
    rows16 = jnp.concatenate(
        [out[0:8, 0:NZ] - out[8:16, NZ:], out[0:8, NZ:] + out[8:16, 0:NZ]], axis=0
    )
    row16 = lax.broadcasted_iota(jnp.int32, (16, 128), 0)
    lane16 = lax.broadcasted_iota(jnp.int32, (16, 128), 1) // 8
    for block in range(4):
        piece = rows16[:, 128 * block : 128 * block + 128]
        for bit in range(4):
            step = 1 << bit
            piece = jnp.where(
                (row16 // step) % 2 == 1, pltpu.roll(piece, 128 - 8 * step, 1), piece
            )
        for bit in range(4):
            step = 1 << bit
            piece = jnp.where((lane16 // step) % 2 == 1, pltpu.roll(piece, step, 0), piece)
        for g in range(16):
            csend[16 * block + g] = piece[g : g + 1]

    for i in range(PEERS - 1, 0, -1):
        peer = me ^ i
        pltpu.make_async_remote_copy(
            src_ref=csend.at[peer],
            dst_ref=crecv.at[me],
            send_sem=misc_sem.at[6],
            recv_sem=misc_sem.at[7],
            device_id=(peer, slab),
            device_id_type=MESH,
        ).start()
    crecv[me] = csend[me]
    left_device(crecv, misc_sem.at[7], PEERS - 1)
    plane = jnp.broadcast_to(crecv[...], (PEERS, 8, 128)).reshape(KX, 128)
    plane = pltpu.roll(plane, lax.rem(128 - 8 * lax.rem(me, 16), 128), 1)
    rank = lax.broadcasted_iota(jnp.int32, (KX, 128), 0)
    for bit in range(3):
        step = 1 << bit
        plane = jnp.where((rank // step) % 2 == 1, pltpu.roll(plane, 8 * step, 1), plane)
    plane = x_part(plane)
    for b in range(4):
        turned = plane[128 * b : 128 * b + 128, :].T
        fsend[b] = turned[0:8]
        fsend[4 + b] = turned[64:72]
    to_slabs(
        lambda peer: fsend.at[peer], frecv.at[slab], misc_sem.at[2], misc_sem.at[3]
    )
    frecv[slab] = fsend[slab]
    left_device(frecv, misc_sem.at[3], SLABS - 1)
    total = frecv[0]
    for b in range(1, SLABS):
        total = total + frecv[b]
    out_grad[...] = total

    @pl.loop(0, 7)
    def _(slot):
        left_device(send.at[slot], send_sem.at[slot], PEERS - 1)

    @pl.loop(0, ROUNDS)
    def _(r):
        left_device(srecv.at[r], ssend_sem.at[r], SLABS - 1)
        for side in range(2):
            @pl.when(r != 2)
            def _():
                whole = hsend.at[r, side]
                pltpu.make_async_copy(whole, whole, hsend_sem.at[r, side]).wait()

            @pl.when(r == 2)
            def _():
                whole = hsend.at[r, side, pl.ds(0, 1)]
                pltpu.make_async_copy(whole, whole, hsend_sem.at[r, side]).wait()

    left_device(grecv, misc_sem.at[0], SLABS - 1)
    pltpu.make_async_copy(corner, corner, misc_sem.at[4]).wait()
    left_device(frecv, misc_sem.at[2], SLABS - 1)
    left_device(crecv, misc_sem.at[6], PEERS - 1)


def per_device(initial_state, drag_rate, wall_control, lift_profile, schur_inverse):
    row = (2, MODES, NZ)
    vmem = pl.BlockSpec(memory_space=pltpu.VMEM)
    hbm = pl.BlockSpec(memory_space=pl.ANY)
    smem = pl.BlockSpec(memory_space=pltpu.SMEM)
    dma = pltpu.SemaphoreType.DMA
    return pl.pallas_call(
        kernel,
        out_shape=(
            jax.ShapeDtypeStruct((3, 2, ROWS, MODES, NZ), F32),
            jax.ShapeDtypeStruct((8, 128), F32),
        ),
        in_specs=[hbm, hbm, hbm, smem, hbm, hbm, hbm],
        out_specs=(hbm, vmem),
        scratch_shapes=[
            pltpu.VMEM((3, ROWS + 4, *row), F32),
            pltpu.VMEM((ROWS, *row), F32),
            pltpu.VMEM((ROWS + 2, *row), F32),
            pltpu.VMEM((ROWS, *row), F32),
            pltpu.VMEM((ROWS, *row), F32),
            pltpu.VMEM((ROWS, *row), F32),
            pltpu.VMEM((ROWS + 2, *row), F32),
            pltpu.VMEM(row, F32),
            pltpu.VMEM(row, F32),
            pltpu.VMEM((ROWS, *row), F32),
            pltpu.VMEM((ROWS, *row), F32),
            pltpu.VMEM((ROWS, ROWS, MODES, NZ), F32),
            pltpu.VMEM((ROWS, MODES, NX), F32),
            pltpu.VMEM((8, NX), F32),
            pltpu.VMEM((96, 512), F32),
            pltpu.VMEM((96, 512), F32),
            pltpu.VMEM((1024, 1024), BF16),
            pltpu.VMEM((2, 1024, 512), BF16),
            pltpu.VMEM((512, 1024), BF16),
            pltpu.VMEM((512, 1024), BF16),
            pltpu.VMEM((512, 128), F32),
            pltpu.VMEM((4, MODES, NZ), F32),
            pltpu.VMEM((MODES, NZ), F32),
            pltpu.VMEM((7, PEERS, 8, 128), F32),
            pltpu.VMEM((7, PEERS, 8, 128), F32),
            pltpu.VMEM((ROUNDS, 2, 4, *row), F32),
            pltpu.VMEM((ROUNDS, 2, 4, *row), F32),
            pltpu.VMEM((ROUNDS, 2, *row), F32),
            pltpu.VMEM((ROUNDS, SLABS, *row), F32),
            pltpu.VMEM((4, MODES, NZ), F32),
            pltpu.VMEM((SLABS, 3, MODES, NZ), F32),
            pltpu.VMEM((MODES, NZ), F32),
            pltpu.VMEM((SLABS, 8, 128), F32),
            pltpu.VMEM((SLABS, 8, 128), F32),
            pltpu.VMEM((PEERS, 1, 128), F32),
            pltpu.VMEM((PEERS, 1, 128), F32),
            dma((7,)),
            dma((7, 2)),
            dma((ROUNDS, 2)),
            dma((ROUNDS, 2)),
            dma((ROUNDS,)),
            dma((ROUNDS,)),
            dma((8,)),
            dma((17,)),
        ],
        compiler_params=pltpu.CompilerParams(
            collective_id=0, has_side_effects=True, vmem_limit_bytes=60 * 1024 * 1024
        ),
        name="channel_adjoint",
    )(
        initial_state,
        drag_rate,
        wall_control,
        lift_profile,
        schur_inverse,
        jnp.asarray(base_table(NX, 1.0 / math.sqrt(NX))),
        jnp.asarray(base_table(NZ, 1.0 / math.sqrt(NZ))),
    )


def solution(mesh):
    return jax.shard_map(
        per_device,
        mesh=mesh,
        in_specs=(
            P(None, None, "gy", "xz", None),
            P("gy", "xz", None),
            P("xz", None),
            P(),
            P("gy", None, "xz", None),
        ),
        out_specs=(P(None, None, "gy", "xz", None), P("xz", "gy")),
        check_vma=False,
    )
```

```python
import functools
import math

import jax
import jax.numpy as jnp
import numpy as np
from jax import lax
from jax.experimental import pallas as pl
from jax.experimental.pallas import tpu as pltpu
from jax.sharding import PartitionSpec as P

MESH = pl.DeviceIdType.MESH
F32 = jnp.float32
BF16 = jnp.bfloat16
DIFFUSION = 0.04
NX = 1024
NZ = 512
KX = 512
ROWS = 8
MODES = 8
PEERS = 64
SLABS = 8
ROUNDS = 4
CONTROL_SLOT = 6
ORDER = (0, 1)


def base_table(period, scale):
    k = np.arange(512)
    high = 2.0 * np.pi * ((32 * np.arange(16)[:, None] * k) % period) / period
    low = 2.0 * np.pi * ((np.arange(32)[:, None] * k) % period) / period
    return np.concatenate(
        [np.cos(high), np.sin(high), np.cos(low) * scale, np.sin(low) * scale]
    ).astype(np.float32)


def split(x):
    hi = x.astype(BF16)
    return hi, (x - hi.astype(F32))


def regrouped(tiles, lane):
    tiles = [pltpu.roll(tiles[-j % 16], 8 * (-j % 16), 1) if j else tiles[0] for j in range(16)]
    for bit in range(4):
        step = 1 << bit
        chosen = (lane // (8 * step)) % 2 == 1
        tiles = [jnp.where(chosen, tiles[(g - step) % 16], tiles[g]) for g in range(16)]
    return [pltpu.roll(tile, 128 - 8 * g, 1) if g else tile for g, tile in enumerate(tiles)]


def kernel(
    state_hbm, drag_hbm, ctrl_hbm, lift_ref, schur_hbm, base_x_hbm, base_z_hbm,
    out_state, out_grad,
    st, pu, pv, pw, divb, direct, pbuf, wall, chat, zin, zout,
    schur, drag_in, ctrl_in, base_x, base_z, txi, tx, tzh, tzl, dg, waves, amat,
    send, recv, hsend, hrecv, ssend, srecv, gsend, grecv, corner, fsend, frecv, csend, crecv,
    send_sem, recv_sem, hsend_sem, hrecv_sem, ssend_sem, srecv_sem, misc_sem, load_sem,
):
    me = lax.axis_index("xz")
    slab = lax.axis_index("gy")
    barrier = pltpu.get_barrier_semaphore()
    for i in range(PEERS - 1, 0, -1):
        pl.semaphore_signal(barrier, inc=1, device_id=(me ^ i, slab), device_id_type=MESH)
    for i in (4, 3, 5, 2, 6, 1, 7):
        pl.semaphore_signal(
            barrier, inc=1, device_id=(me, lax.rem(slab + i, SLABS)), device_id_type=MESH
        )
    loads = [pltpu.make_async_copy(base_z_hbm, base_z, load_sem.at[0])]
    for comp in range(3):
        for c in range(2):
            loads.append(
                pltpu.make_async_copy(
                    state_hbm.at[comp, c],
                    st.at[comp, pl.ds(2, ROWS), c],
                    load_sem.at[1 + 2 * comp + c],
                )
            )
    for k, (source, target) in enumerate(
        ((base_x_hbm, base_x), (drag_hbm, drag_in), (ctrl_hbm, ctrl_in), (schur_hbm, schur))
    ):
        loads.append(pltpu.make_async_copy(source, target, load_sem.at[7 + k]))
    for load in loads:
        load.start()
    stores = [
        pltpu.make_async_copy(
            st.at[comp, pl.ds(2, ROWS), c],
            out_state.at[comp, c],
            load_sem.at[11 + 2 * comp + c],
        )
        for comp in range(3)
        for c in range(2)
    ]

    lane = lax.broadcasted_iota(jnp.int32, (8, 128), 1)
    wide_lane = lax.broadcasted_iota(jnp.int32, (KX, 128), 1)
    left = wide_lane < 64
    left_half = left[0:256]
    odd_half = lax.broadcasted_iota(jnp.int32, (256, 128), 0) % 2 == 1
    odd = lax.broadcasted_iota(jnp.int32, (KX, 128), 0) % 2 == 1

    mode = me * MODES + lax.broadcasted_iota(jnp.int32, (MODES, NZ), 0)
    span = lax.broadcasted_iota(jnp.int32, (MODES, NZ), 1)
    kx = (2.0 * math.pi / NX) * mode.astype(F32)
    signed = jnp.where(span < NZ // 2, span, span - NZ)
    kz = jnp.where(span == NZ // 2, 0.0, (2.0 * math.pi / NZ) * signed.astype(F32))
    waves[0] = kx
    waves[1] = kz
    waves[2] = kx * kx + kz * kz
    waves[3] = jnp.where(mode == 0, 1.0, 2.0).astype(F32)

    def turns(base, i):
        ca = base[pl.ds(i, 1), :]
        sa = base[pl.ds(16 + i, 1), :]
        cb = base[32:64, :]
        sb = base[64:96, :]
        c_hi, c_lo = split(ca * cb - sa * sb)
        s_hi, s_lo = split(sa * cb + ca * sb)
        return c_hi, c_lo.astype(BF16), s_hi, s_lo.astype(BF16)

    loads[0].wait()

    @pl.loop(0, 16)
    def _(i):
        rows = pl.ds(pl.multiple_of(i * 32, 32), 32)
        tzh[rows, 0:512], tzl[rows, 0:512], tzh[rows, 512:1024], tzl[rows, 512:1024] = turns(
            base_z, i
        )

    def prepare():
        loads[7].wait()

        @pl.loop(0, 16)
        def _(i):
            c_hi, c_lo, s_hi, s_lo = turns(base_x, i)
            rows = pl.ds(pl.multiple_of(i * 32, 32), 32)
            low_rows = pl.ds(pl.multiple_of(512 + i * 32, 32), 32)
            txi[rows, 0:512] = c_hi
            txi[rows, 512:1024] = s_hi
            txi[low_rows, 0:512] = c_lo
            txi[low_rows, 512:1024] = s_lo
            for k, part in enumerate((c_hi, c_lo, s_hi, s_lo)):
                start = pl.multiple_of(256 * k + lax.rem(i, 8) * 32, 32)
                tx[i // 8, pl.ds(start, 32)] = part

        loads[8].wait()
        for b in range(4):
            lo = drag_in[:, :, 128 * b : 128 * b + 128].reshape(64, 128)
            hi = drag_in[:, :, 512 + 128 * b : 640 + 128 * b].reshape(64, 128)
            dg[128 * b : 128 * b + 128, :] = jnp.concatenate([lo, hi], axis=0).T

        loads[9].wait()
        for b in range(4):
            near = ctrl_in[:, 128 * b : 128 * b + 128]
            far = ctrl_in[:, 512 + 128 * b : 640 + 128 * b]
            blank = jnp.zeros((56, 128), F32)
            pieces = jnp.concatenate([near, blank, far, blank], axis=0)
            send[CONTROL_SLOT, 16 * b : 16 * b + 16] = pieces.T.reshape(16, 8, 128)
        x_forward(send[CONTROL_SLOT].reshape(KX, 128), CONTROL_SLOT)
        loads[10].wait()
        gsend[0] = schur[0, 7]
        gsend[1] = schur[7, 0]
        gsend[2] = schur[0, 0]
        gsend[3] = schur[7, 7]
        to_slabs(
            lambda peer: gsend.at[pl.ds(0, 3)],
            grecv.at[slab],
            misc_sem.at[0],
            misc_sem.at[1],
        )
        pltpu.make_async_remote_copy(
            src_ref=gsend.at[3],
            dst_ref=corner,
            send_sem=misc_sem.at[4],
            recv_sem=misc_sem.at[5],
            device_id=(me, lax.rem(slab + 1, SLABS)),
            device_id_type=MESH,
        ).start()

    def x_part(value):
        hi = value.astype(BF16).astype(F32)
        lo = value - hi
        real = jnp.where(left, hi, pltpu.roll(lo, 64, 1))
        imag = -jnp.where(left, pltpu.roll(hi, 64, 1), lo)
        rc = jnp.concatenate([real, jnp.where(odd, -real, real)], axis=1)
        rs = jnp.concatenate([imag, jnp.where(odd, -imag, imag)], axis=1)
        both = jnp.concatenate([rc, rs], axis=0).astype(BF16)
        out = jnp.dot(txi[...], both, preferred_element_type=F32)
        out = out[0:KX] + out[KX : 2 * KX]
        near, far = out[:, 0:128], out[:, 128:256]
        near = near + pltpu.roll(near, 64, 1)
        far = far + pltpu.roll(far, 64, 1)
        return jnp.where(left, near, far)

    def x_inverse(slot):
        for hh in ORDER:
            arrived(slot, (me // 32) ^ hh, hh == 0)
        return x_part(recv[slot].reshape(KX, 128))

    def x_forward(value, slot):
        turned = pltpu.roll(value, 64, 1)
        total = value + turned
        gap = jnp.where(left, value - turned, turned - value)

        def packed(part):
            hi = part.astype(BF16).astype(F32)
            return jnp.where(left, hi, part - hi)

        ra = jnp.concatenate([packed(total), packed(gap)], axis=1).astype(BF16)
        def folded(part):
            part = jnp.where(odd_half, part[:, 128:256], part[:, 0:128])
            return part + pltpu.roll(part, 64, 1)

        for hh in (1, 0):
            h = (me // 32) ^ hh
            out = jnp.dot(tx[h], ra, preferred_element_type=F32)
            with_cos = folded(out[0:256] + out[256:512])
            with_sin = folded(out[512:768] + out[768:1024])
            result = jnp.where(left_half, with_cos, -with_sin)
            send[slot, pl.ds(h * 32, 32)] = result.reshape(32, 8, 128)
            exchange(slot, h, hh == 0)

    def z_dot(value, rows):
        count = value.shape[0]
        hi, lo = split(value)
        both = jnp.concatenate([hi, lo.astype(BF16)], axis=0)
        out = jnp.dot(both, tzh[rows, :], preferred_element_type=F32)
        out = out[0:count] + out[count : 2 * count]
        return out + jnp.dot(hi, tzl[rows, :], preferred_element_type=F32)

    def z_inverse(value, slot, sent):
        out = z_dot(value, slice(0, NZ)).reshape(ROWS, 2, MODES, 2 * NZ)
        with_cos, with_sin = out[:, :, :, 0:NZ], out[:, :, :, NZ : 2 * NZ]
        zout[:, 0] = with_cos[:, 0] - with_sin[:, 1]
        zout[:, 1] = with_sin[:, 0] + with_cos[:, 1]

        for hh in (1, 0):
            h = (me // 32) ^ hh
            for j in range(2):
                block = 2 * h + j
                lanes = pl.ds(pl.multiple_of(block * 128, 128), 128)
                tiles = [zout[a % 8, a // 8, :, lanes] for a in range(16)]
                for g, tile in enumerate(regrouped(tiles, lane)):
                    send[slot, block * 16 + g] = tile
            if sent:
                exchange(slot, h, hh == 0)

    def z_forward(slot):
        out = None
        for hh in ORDER:
            h = (me // 32) ^ hh
            arrived(slot, h, hh == 0)
            half = pl.ds(pl.multiple_of(h * 256, 256), 256)
            for j in range(2):
                block = 2 * h + j
                lanes = pl.ds(pl.multiple_of(block * 128, 128), 128)
                tiles = [recv[slot, block * 16 + g] for g in range(16)]
                for a, tile in enumerate(regrouped(tiles, lane)):
                    zin[a % 8, a // 8, :, lanes] = tile
            part = z_dot(zin[:, :, :, half].reshape(128, 256), half)
            out = part if out is None else out + part
        out = out.reshape(ROWS, 2, MODES, 2 * NZ)
        with_cos, with_sin = out[:, :, :, 0:NZ], out[:, :, :, NZ : 2 * NZ]
        zout[:, 0] = with_cos[:, 0] + with_sin[:, 1]
        zout[:, 1] = with_cos[:, 1] - with_sin[:, 0]

    def exchange(slot, h, own):
        order = [8 * y + x for x in (7, 6, 5, 4, 3, 2, 1, 0) for y in ((3, 2, 1, 0) if own else range(4))]
        for i in [k for k in order if k or not own]:
            peer = h * 32 + (lax.rem(me, 32) ^ i)
            pltpu.make_async_remote_copy(
                src_ref=send.at[slot, peer],
                dst_ref=recv.at[slot, me],
                send_sem=send_sem.at[slot],
                recv_sem=recv_sem.at[slot, me // 32],
                device_id=(peer, slab),
                device_id_type=MESH,
            ).start()
        if own:
            recv[slot, me] = send[slot, me]

    def arrived(slot, h, own):
        whole = recv.at[slot, pl.ds(0, 31 if own else 32)]
        pltpu.make_async_copy(whole, whole, recv_sem.at[slot, h]).wait()

    def left_device(buffer, sem, count):
        whole = buffer.at[pl.ds(0, count)]
        pltpu.make_async_copy(whole, whole, sem).wait()

    def to_slabs(source, target, out_sem, in_sem):
        for i in (4, 3, 5, 2, 6, 1, 7):
            peer = lax.rem(slab + i, SLABS)
            pltpu.make_async_remote_copy(
                src_ref=source(peer),
                dst_ref=target,
                send_sem=out_sem,
                recv_sem=in_sem,
                device_id=(me, peer),
                device_id_type=MESH,
            ).start()

    loads[1].wait()
    loads[2].wait()
    z_inverse((st[0, 2:10] * waves[3]).reshape(128, NZ), 0, False)
    pl.semaphore_wait(barrier, PEERS - 1 + SLABS - 1)
    for hh in (1, 0):
        exchange(0, (me // 32) ^ hh, hh == 0)
    wall[...] = jnp.zeros_like(wall)

    @pl.loop(0, ROUNDS)
    def _(r):
        adjoint = r // 2
        moving = r != 2
        rate = jnp.where(moving, DIFFUSION, 0.0).astype(F32)

        @pl.when(r == 0)
        def _():
            for load in loads[3:7]:
                load.wait()

        for side, (u_row, v_row) in enumerate(((9, 8), (2, 2))):
            hsend[r, side, 0] = st[0, u_row]
            hsend[r, side, 1] = st[1, v_row]
            hsend[r, side, 2] = st[1, v_row + 1]
            hsend[r, side, 3] = st[2, u_row]
        def send_halo(part):
            for side in range(2):
                rows = part(side)
                pltpu.make_async_remote_copy(
                    src_ref=hsend.at[r, side, rows],
                    dst_ref=hrecv.at[r, side, rows],
                    send_sem=hsend_sem.at[r, side],
                    recv_sem=hrecv_sem.at[r, side],
                    device_id=(me, lax.rem(slab + (1 if side == 0 else SLABS - 1), SLABS)),
                    device_id_type=MESH,
                ).start()

        def wait_halo(part, buffer, sem):
            for side in range(2):
                whole = buffer.at[r, side, part(side)]
                pltpu.make_async_copy(whole, whole, sem.at[r, side]).wait()

        def all_rows(side):
            return pl.ds(0, 4)

        def near_row(side):
            return pl.ds(2 - side, 1)

        @pl.when(moving)
        def _():
            send_halo(all_rows)

        @pl.when(r == 2)
        def _():
            send_halo(near_row)

        @pl.when(jnp.logical_or(r == 1, r == 3))
        def _():
            before = jnp.where(r < 2, waves[3], 1.0)
            value = (st[0, 2:10] * before).reshape(128, NZ)
            z_inverse(value, 2 * jnp.where(r == 3, 2, r), True)

        @pl.when(r == 0)
        def _():
            prepare()

        @pl.when(moving)
        def _():
            wait_halo(all_rows, hrecv, hrecv_sem)
            for side, (u_row, v_row, edge) in enumerate(((1, 0, 0), (10, 10, SLABS - 1))):
                open_side = slab != edge
                st[0, u_row] = jnp.where(open_side, hrecv[r, side, 0], 0.0)
                st[1, v_row] = jnp.where(open_side, hrecv[r, side, 1], 0.0)
                st[1, v_row + 1] = jnp.where(open_side, hrecv[r, side, 2], 0.0)
                st[2, u_row] = jnp.where(open_side, hrecv[r, side, 3], 0.0)

        @pl.when(r == 2)
        def _():
            st[1, 1] = jnp.zeros((2, MODES, NZ), F32)
            st[1, 10] = jnp.zeros((2, MODES, NZ), F32)

        square = waves[2]

        def diffused(comp, row):
            middle = st[comp, row]
            around = st[comp, row + 1] - 2.0 * middle + st[comp, row - 1]
            return middle + rate * (around - square * middle)

        @pl.loop(0, ROWS)
        def _(y):
            pu[y] = diffused(0, y + 2)
            pw[y] = diffused(2, y + 2)

        @pl.loop(0, ROWS + 2)
        def _(y):
            row = slab * ROWS + y - 1
            inside = jnp.logical_and(row >= 0, row < ROWS * SLABS)
            pv[y] = jnp.where(inside, diffused(1, y + 1), 0.0)

        @pl.when(moving)
        def _():
            slot = 2 * jnp.where(r == 3, 2, r)
            x_forward(x_inverse(slot) * dg[...], slot + 1)

        @pl.when(r == 0)
        def _():
            z_forward(CONTROL_SLOT)
            chat[...] = zout[0]
            pltpu.make_async_copy(
                grecv.at[pl.ds(0, SLABS - 1)], grecv.at[pl.ds(0, SLABS - 1)], misc_sem.at[1]
            ).wait()
            pltpu.make_async_copy(corner, corner, misc_sem.at[5]).wait()

            def gather_a(i, a):
                b = SLABS - 1 - i
                return grecv[b, 2] + grecv[b, 0] * a * grecv[b, 1]

            amat[...] = lax.fori_loop(0, SLABS - 1 - slab, gather_a, jnp.zeros((MODES, NZ), F32))

        @pl.when(r < 2)
        def _():
            @pl.loop(0, ROWS + 2)
            def _(y):
                row = slab * ROWS + y - 1
                inside = jnp.logical_and(row >= 0, row < ROWS * SLABS)
                safe = jnp.clip(row, 0, ROWS * SLABS - 1)
                level = jnp.where(inside, lift_ref[safe], 0.0)
                pv[y] = pv[y] + level * chat[...]

        kxv, kzv = waves[0], waves[1]

        @pl.when(moving)
        def _():
            slot = 2 * jnp.where(r == 3, 2, r) + 1
            z_forward(slot)
            after = jnp.where(r < 2, 1.0, waves[3])

            @pl.loop(0, ROWS)
            def _(y):
                pu[y] = pu[y] - zout[y] * after

        @pl.loop(0, ROWS)
        def _(y):
            slope = 0.5 * (pv[y + 2] - pv[y])
            divb[y, 0] = slope[0] - kxv * pu[y, 1] - kzv * pw[y, 1]
            divb[y, 1] = slope[1] + kxv * pu[y, 0] + kzv * pw[y, 0]

        def entry(i, j):
            return schur[i + adjoint * (j - i), j + adjoint * (i - j)]

        def solve_row(i):
            total = entry(i, 0) * divb[0]
            for j in range(1, ROWS):
                total = total + entry(i, j) * divb[j]
            direct[i] = total

        @pl.loop(0, 2)
        def _(i):
            solve_row(7 * i)

        ratio = entry(7, 0)
        turn = entry(0, 7)
        half = jnp.where(r == 2, 0.5, 0.0).astype(F32)
        last = direct[7] - half * st[1, 9]
        first_v = half * st[1, 2]
        cross = jnp.where(slab == 0, 0.0, corner[...] * first_v)
        ssend[r, 0] = last + ratio * cross
        ssend[r, 1] = (
            direct[0]
            + turn * (amat[...] * last)
            + first_v
            + (schur[0, 0] + turn * amat[...] * ratio) * cross
        )
        to_slabs(
            lambda peer: ssend.at[r, jnp.where(peer > slab, 0, 1)],
            srecv.at[r, slab],
            ssend_sem.at[r],
            srecv_sem.at[r],
        )

        @pl.loop(1, ROWS - 1)
        def _(i):
            solve_row(i)

        whole = srecv.at[r, pl.ds(0, SLABS - 1)]
        pltpu.make_async_copy(whole, whole, srecv_sem.at[r]).wait()

        blank = jnp.zeros((2, MODES, NZ), F32)
        entering = lax.fori_loop(
            0, slab, lambda b, z: srecv[r, b] + grecv[b, 1 - adjoint] * z, blank
        )
        entering = entering + cross

        def suffix(i, e):
            b = SLABS - 1 - i
            return srecv[r, b] + grecv[b, adjoint] * e

        above = lax.fori_loop(0, SLABS - 1 - slab, suffix, blank)
        leaving = above + amat[...] * (last + ratio * entering)
        pbuf[9] = leaving

        @pl.loop(0, ROWS)
        def _(i):
            pbuf[i + 1] = direct[i] + entry(i, 0) * entering + entry(i, 7) * leaving

        pbuf[0] = jnp.where(slab == 0, 0.0, entering + corner[...] * pbuf[1])

        @pl.when(r == 2)
        def _():
            wait_halo(near_row, hrecv, hrecv_sem)
            pbuf[0] = pbuf[0] + jnp.where(slab == 0, 0.0, 0.5 * hrecv[r, 0, 2])
            pbuf[9] = pbuf[9] - jnp.where(slab == SLABS - 1, 0.0, 0.5 * hrecv[r, 1, 1])
            for copy in stores:
                copy.wait()

        @pl.loop(0, ROWS)
        def _(y):
            p0, p1 = pbuf[y + 1, 0], pbuf[y + 1, 1]
            st[0, y + 2, 0] = pu[y, 0] + kxv * p1
            st[0, y + 2, 1] = pu[y, 1] - kxv * p0
            st[2, y + 2, 0] = pw[y, 0] + kzv * p1
            st[2, y + 2, 1] = pw[y, 1] - kzv * p0
            normal = pv[y + 1] - 0.5 * (pbuf[y + 2] - pbuf[y])
            st[1, y + 2] = normal
            level = jnp.where(r >= 2, lift_ref[slab * ROWS + y], 0.0)
            wall[...] = wall[...] + level * normal

        @pl.when(r == 1)
        def _():
            for copy in stores:
                copy.start()

    out = z_dot(wall[...].reshape(16, NZ), slice(0, NZ))
    rows16 = jnp.concatenate(
        [out[0:8, 0:NZ] - out[8:16, NZ:], out[0:8, NZ:] + out[8:16, 0:NZ]], axis=0
    )
    row16 = lax.broadcasted_iota(jnp.int32, (16, 128), 0)
    lane16 = lax.broadcasted_iota(jnp.int32, (16, 128), 1) // 8
    for block in range(4):
        piece = rows16[:, 128 * block : 128 * block + 128]
        for bit in range(4):
            step = 1 << bit
            piece = jnp.where(
                (row16 // step) % 2 == 1, pltpu.roll(piece, 128 - 8 * step, 1), piece
            )
        for bit in range(4):
            step = 1 << bit
            piece = jnp.where((lane16 // step) % 2 == 1, pltpu.roll(piece, step, 0), piece)
        for g in range(16):
            csend[16 * block + g] = piece[g : g + 1]

    for i in [8 * y + x for x in range(8) for y in range(8)][:0:-1]:
        peer = me ^ i
        pltpu.make_async_remote_copy(
            src_ref=csend.at[peer],
            dst_ref=crecv.at[me],
            send_sem=misc_sem.at[6],
            recv_sem=misc_sem.at[7],
            device_id=(peer, slab),
            device_id_type=MESH,
        ).start()
    crecv[me] = csend[me]
    left_device(crecv, misc_sem.at[7], PEERS - 1)
    plane = jnp.broadcast_to(crecv[...], (PEERS, 8, 128)).reshape(KX, 128)
    plane = pltpu.roll(plane, lax.rem(128 - 8 * lax.rem(me, 16), 128), 1)
    rank = lax.broadcasted_iota(jnp.int32, (KX, 128), 0)
    for bit in range(3):
        step = 1 << bit
        plane = jnp.where((rank // step) % 2 == 1, pltpu.roll(plane, 8 * step, 1), plane)
    plane = x_part(plane)
    for b in range(4):
        turned = plane[128 * b : 128 * b + 128, :].T
        fsend[b] = turned[0:8]
        fsend[4 + b] = turned[64:72]
    to_slabs(
        lambda peer: fsend.at[peer], frecv.at[slab], misc_sem.at[2], misc_sem.at[3]
    )
    frecv[slab] = fsend[slab]
    left_device(frecv, misc_sem.at[3], SLABS - 1)
    total = frecv[0]
    for b in range(1, SLABS):
        total = total + frecv[b]
    out_grad[...] = total

    @pl.loop(0, 7)
    def _(slot):
        left_device(send.at[slot], send_sem.at[slot], PEERS - 1)

    @pl.loop(0, ROUNDS)
    def _(r):
        left_device(srecv.at[r], ssend_sem.at[r], SLABS - 1)
        for side in range(2):
            @pl.when(r != 2)
            def _():
                whole = hsend.at[r, side]
                pltpu.make_async_copy(whole, whole, hsend_sem.at[r, side]).wait()

            @pl.when(r == 2)
            def _():
                whole = hsend.at[r, side, pl.ds(0, 1)]
                pltpu.make_async_copy(whole, whole, hsend_sem.at[r, side]).wait()

    left_device(grecv, misc_sem.at[0], SLABS - 1)
    pltpu.make_async_copy(corner, corner, misc_sem.at[4]).wait()
    left_device(frecv, misc_sem.at[2], SLABS - 1)
    left_device(crecv, misc_sem.at[6], PEERS - 1)


def per_device(initial_state, drag_rate, wall_control, lift_profile, schur_inverse):
    row = (2, MODES, NZ)
    vmem = pl.BlockSpec(memory_space=pltpu.VMEM)
    hbm = pl.BlockSpec(memory_space=pl.ANY)
    smem = pl.BlockSpec(memory_space=pltpu.SMEM)
    dma = pltpu.SemaphoreType.DMA
    return pl.pallas_call(
        kernel,
        out_shape=(
            jax.ShapeDtypeStruct((3, 2, ROWS, MODES, NZ), F32),
            jax.ShapeDtypeStruct((8, 128), F32),
        ),
        in_specs=[hbm, hbm, hbm, smem, hbm, hbm, hbm],
        out_specs=(hbm, vmem),
        scratch_shapes=[
            pltpu.VMEM((3, ROWS + 4, *row), F32),
            pltpu.VMEM((ROWS, *row), F32),
            pltpu.VMEM((ROWS + 2, *row), F32),
            pltpu.VMEM((ROWS, *row), F32),
            pltpu.VMEM((ROWS, *row), F32),
            pltpu.VMEM((ROWS, *row), F32),
            pltpu.VMEM((ROWS + 2, *row), F32),
            pltpu.VMEM(row, F32),
            pltpu.VMEM(row, F32),
            pltpu.VMEM((ROWS, *row), F32),
            pltpu.VMEM((ROWS, *row), F32),
            pltpu.VMEM((ROWS, ROWS, MODES, NZ), F32),
            pltpu.VMEM((ROWS, MODES, NX), F32),
            pltpu.VMEM((8, NX), F32),
            pltpu.VMEM((96, 512), F32),
            pltpu.VMEM((96, 512), F32),
            pltpu.VMEM((1024, 1024), BF16),
            pltpu.VMEM((2, 1024, 512), BF16),
            pltpu.VMEM((512, 1024), BF16),
            pltpu.VMEM((512, 1024), BF16),
            pltpu.VMEM((512, 128), F32),
            pltpu.VMEM((4, MODES, NZ), F32),
            pltpu.VMEM((MODES, NZ), F32),
            pltpu.VMEM((7, PEERS, 8, 128), F32),
            pltpu.VMEM((7, PEERS, 8, 128), F32),
            pltpu.VMEM((ROUNDS, 2, 4, *row), F32),
            pltpu.VMEM((ROUNDS, 2, 4, *row), F32),
            pltpu.VMEM((ROUNDS, 2, *row), F32),
            pltpu.VMEM((ROUNDS, SLABS, *row), F32),
            pltpu.VMEM((4, MODES, NZ), F32),
            pltpu.VMEM((SLABS, 3, MODES, NZ), F32),
            pltpu.VMEM((MODES, NZ), F32),
            pltpu.VMEM((SLABS, 8, 128), F32),
            pltpu.VMEM((SLABS, 8, 128), F32),
            pltpu.VMEM((PEERS, 1, 128), F32),
            pltpu.VMEM((PEERS, 1, 128), F32),
            dma((7,)),
            dma((7, 2)),
            dma((ROUNDS, 2)),
            dma((ROUNDS, 2)),
            dma((ROUNDS,)),
            dma((ROUNDS,)),
            dma((8,)),
            dma((17,)),
        ],
        compiler_params=pltpu.CompilerParams(
            collective_id=0, has_side_effects=True, vmem_limit_bytes=60 * 1024 * 1024
        ),
        name="channel_adjoint",
    )(
        initial_state,
        drag_rate,
        wall_control,
        lift_profile,
        schur_inverse,
        jnp.asarray(base_table(NX, 1.0 / math.sqrt(NX))),
        jnp.asarray(base_table(NZ, 1.0 / math.sqrt(NZ))),
    )


def solution(mesh):
    return jax.shard_map(
        per_device,
        mesh=mesh,
        in_specs=(
            P(None, None, "gy", "xz", None),
            P("gy", "xz", None),
            P("xz", None),
            P(),
            P("gy", None, "xz", None),
        ),
        out_specs=(P(None, None, "gy", "xz", None), P("xz", "gy")),
        check_vma=False,
    )
```
